32 devices in a mesh: owner: 4 (over y, x), rows: 8 (over z, core).
Axes of the slice: x: 2, y: 2, z: 4, core: 2. Of those that a mesh axis runs over, the one named last changes fastest.
Arguments:
- train_gate: float32 [64, 2048, 1024], P('owner', 'rows'), may hold values from -0.1875 to 0.1875
- train_up: float32 [64, 2048, 1024], P('owner', 'rows'), may hold values from -0.1875 to 0.1875
- train_down: float32 [64, 1024, 2048], P('owner', None, 'rows'), may hold values from -0.25 to 0.25
- router_weight: float32 [2048, 64], P('rows', 'owner'), may hold values from -0.125 to 0.125
- router_gain: float32 [2048], P('rows'), may hold values from 0.25 to 1.75
Outputs:
- ready_gate: bfloat16 [64, 2048, 1024], P('owner', None, 'rows')
- ready_up: bfloat16 [64, 2048, 1024], P('owner', None, 'rows')
- ready_down: bfloat16 [64, 1024, 2048], P('owner', 'rows')
- scale_gate: float32 [64, 1024], P('owner', 'rows')
- scale_up: float32 [64, 1024], P('owner', 'rows')
- scale_down: float32 [64, 1024], P('owner', 'rows')
- serve_router: bfloat16 [2048, 64], replicated
The draws below stay inside these ranges and needn't reach their ends.
All inputs are finite; a program needn't handle non-finite values. Where the reference program divides by a largest or mean magnitude, that divisor is 1e-20 or more.
Results may differ from the reference program's by a relative error of at most 0.0013.
Values may be sent and summed in bfloat16 or wider, within the bound.
A program may use at most 192 MiB of HBM per device.

```python
import jax
import jax.numpy as jnp

EXPERTS = 64
D_MODEL = 2048
D_EXPERT = 1024


def raised(drawn, own_key, source, target, parts, factor):
    owner, partner = [(jnp.arange(drawn.shape[axis_at]) // (drawn.shape[axis_at] // parts)).reshape([-1 if axis == axis_at else 1 for axis in range(drawn.ndim)]) for axis_at in (source, target)]
    chosen = jax.random.permutation(own_key, parts)[partner]
    strong = (owner == chosen) | (owner == (partner + parts // 2) % parts)
    return jnp.where(strong, factor * drawn, drawn)


def steps_of(rng, dims, shards, low, top_value):
    def one(dim, parts):
        heights = jax.random.uniform(jax.random.fold_in(jax.random.fold_in(rng, 6), dim), (parts,), jnp.float32, low / len(shards), top_value / len(shards))
        return jnp.repeat(jnp.exp(heights), dims[dim] // parts).reshape((-1,) + (1,) * (len(dims) - dim - 1))

    factor_of = one(*shards[0])
    for cut in shards[1:]:
        factor_of = factor_of * one(*cut)
    return factor_of


def bell_draw(own_key, shape, scale, reach, pieces=(), dtype=jnp.bfloat16):
    result = scale * jax.random.normal(own_key, shape, jnp.float32)
    if pieces:
        result = result * steps_of(own_key, shape, pieces, -0.22, 0.18)
    return jnp.clip(result, -reach, reach).astype(dtype)


def bell_draw_with(own_key, dims, deviation, reach, split, heavy, kind=jnp.bfloat16):
    result = deviation * jax.random.normal(own_key, dims, jnp.float32)
    if split:
        result = result * steps_of(own_key, dims, split, -0.22, 0.18)
    return jnp.clip(raised(result, jax.random.fold_in(own_key, 3), *heavy), -reach, reach).astype(kind)


def setup_inputs(seed: int = 0) -> dict:
    splits = jax.random.split(jax.random.key(seed), 6)
    train_gate = bell_draw_with(splits[0], (EXPERTS, D_MODEL, D_EXPERT), D_MODEL ** -0.5, 0.1875, ((0, 4), (1, 8)), (1, 2, 8, 2.0), jnp.float32)
    train_up = bell_draw_with(splits[1], (EXPERTS, D_MODEL, D_EXPERT), D_MODEL ** -0.5, 0.1875, ((0, 4), (1, 8)), (1, 2, 8, 2.0), jnp.float32)
    train_down = bell_draw_with(splits[2], (EXPERTS, D_EXPERT, D_MODEL), D_EXPERT ** -0.5, 0.25, ((0, 4), (2, 8)), (2, 1, 8, 2.0), jnp.float32)
    router_weight = bell_draw(splits[3], (D_MODEL, EXPERTS), D_MODEL ** -0.5, 0.125, ((0, 8), (1, 4)), jnp.float32)
    router_gain = jnp.clip(1.0 + 0.15 * jax.random.normal(splits[4], (D_MODEL,), jnp.float32), 0.25, 1.75)
    return {"train_gate": train_gate, "train_up": train_up, "train_down": train_down, "router_weight": router_weight, "router_gain": router_gain}


def reference(train_gate, train_up, train_down, router_weight, router_gain):
    scale_gate = jnp.sum(jnp.abs(train_gate), axis=1) / D_MODEL
    ready_gate = (train_gate / jnp.expand_dims(scale_gate, 1)).astype(jnp.bfloat16)
    scale_up = jnp.sum(jnp.abs(train_up), axis=1) / D_MODEL
    ready_up = (train_up / jnp.expand_dims(scale_up, 1)).astype(jnp.bfloat16)
    scale_down = jnp.sum(jnp.abs(train_down), axis=2) / D_MODEL
    ready_down = (train_down / jnp.expand_dims(scale_down, 2)).astype(jnp.bfloat16)
    serve_router = (router_weight * router_gain[:, None]).astype(jnp.bfloat16)
    return ready_gate, ready_up, ready_down, scale_gate, scale_up, scale_down, serve_router
```

```python
import functools

import jax
import jax.numpy as jnp
from jax import lax
from jax.experimental import pallas as pl
from jax.experimental.pallas import tpu as pltpu
from jax.sharding import PartitionSpec as P

CORES = 2
SLOTS = 4
EARLY = 2
GROUPS = 4
MESH = pl.DeviceIdType.MESH


def groups_of(experts, start):
    per = max(1, experts // GROUPS)
    out = [(e, 1) for e in range(start)]
    at = start
    while at < experts:
        end = min(experts, (at // per + 1) * per)
        out.append((at, end - at))
        at = end
    return out


def plan(experts):
    early = min(EARLY, experts // 2)
    groups = [groups_of(experts, early), groups_of(experts, 0), groups_of(experts, 0)]
    base = [0, len(groups[0]), len(groups[0]) + len(groups[1])]
    return early, groups, base, sum(len(g) for g in groups)


def exchange(
    n,
    owners,
    gate,
    up,
    down,
    router_weight,
    router_gain,
    out_gate,
    out_up,
    out_down,
    scale_gate,
    scale_up,
    scale_down,
    out_router,
    first,
    wide,
    tall,
    send_wide,
    send_tall,
    early_part,
    early_got,
    early_inv,
    part,
    got_side,
    half_sum,
    got_half,
    total,
    inverse,
    weight,
    gain,
    router,
    load_sem,
    early_send,
    early_recv,
    side_send,
    side_recv,
    half_send,
    half_recv,
    total_send,
    total_recv,
    router_send,
    router_recv,
    fwd_send,
    fwd_recv,
    col_send,
    col_recv,
    bulk_send,
    bulk_recv,
):
    me = lax.axis_index("rows")
    home = lax.axis_index("owner")
    experts, rows, width = gate.shape
    share = width // n
    pair = 2 * share
    half = n // 2
    slots = wide.shape[0]
    chips = n // CORES
    half_chips = chips // 2
    chip = me // CORES
    core = lax.rem(me, CORES)
    side = me // half
    member = lax.rem(me, half)
    facing = lax.rem(me + half, n)
    early, groups, base, _ = plan(experts)
    count = rows * n
    srcs = (gate, up, down)
    span = pl.ds(pl.multiple_of(me * rows, rows), rows)

    def peer(k):
        return lax.rem(me + k, n)

    def mate(k):
        return lax.rem(member + k, half)

    def remote(src, dst, out_sem, in_sem, **where):
        return pltpu.make_async_remote_copy(
            src_ref=src,
            dst_ref=dst,
            send_sem=out_sem,
            recv_sem=in_sem,
            device_id=where,
            device_id_type=MESH,
        )

    def load(t, e):
        buf = wide if t < 2 else tall
        slot = lax.rem(e, slots)
        return pltpu.make_async_copy(
            srcs[t].at[e], buf.at[slot], load_sem.at[0 if t < 2 else 1, slot]
        )

    def load_first(e):
        return pltpu.make_async_copy(gate.at[e], first.at[e], load_sem.at[2, e])

    for e in range(early):
        load_first(e).start()

    def fill(t, start):
        for e in range(start, min(start + slots, experts)):
            load(t, e).start()

    def take(t, e, body):
        load(t, e).wait()
        body(e, lax.rem(e, slots))

        @pl.when(e + slots < experts)
        def _():
            load(t, e + slots).start()

    def run(t, start, stop, body):
        @pl.loop(start, stop)
        def _(e):
            take(t, e, body)

    fill(0, early)
    weight_load = pltpu.make_async_copy(router_weight, weight, load_sem.at[3, 0])
    gain_load = pltpu.make_async_copy(router_gain, gain, load_sem.at[3, 1])
    weight_load.start()
    gain_load.start()

    barrier = pltpu.get_barrier_semaphore()
    for k in range(1, n):
        pl.semaphore_signal(barrier, inc=1, device_id={"rows": peer(k)}, device_id_type=MESH)
    for k in range(1, owners):
        pl.semaphore_signal(
            barrier, inc=1, device_id={"owner": lax.rem(home + k, owners)}, device_id_type=MESH
        )

    def put_part(t, e, sums):
        for q in range(half):
            part[q, t, pl.ds(e, 1), :] = sums[:, q * pair : (q + 1) * pair]

    def sums_wide(t):
        def body(e, slot):
            put_part(t, e, jnp.sum(jnp.abs(wide[slot]), axis=0, keepdims=True))

        return body

    def sums_tall(e, slot):
        for q in range(half):
            block = jnp.abs(tall[slot, q * pair : (q + 1) * pair, :])
            folded = block[:, :128]
            for c in range(128, rows, 128):
                folded = folded + block[:, c : c + 128]
            part[q, 2, pl.ds(e, 1), :] = jnp.sum(folded.T, axis=0, keepdims=True)

    for e in range(early):
        load_first(e).wait()
        sums = jnp.sum(jnp.abs(first[e]), axis=0, keepdims=True)
        put_part(0, e, sums)
        for s in range(2):
            early_part[s, pl.ds(e, 1), :] = sums[:, s * (width // 2) : (s + 1) * (width // 2)]

    pl.semaphore_wait(barrier, n - 1 + owners - 1)

    def early_copy(to, src):
        return remote(
            early_part.at[1 - to // half],
            early_got.at[src],
            early_send.at[to],
            early_recv.at[src],
            rows=to,
        )

    for k in range(1, n):
        early_copy(peer(k), me).start()

    run(0, early, experts, sums_wide(0))

    stages = (pl.ds(0, 1), pl.ds(1, 2))

    def side_copy(s, to, src):
        return remote(
            part.at[to, stages[s]],
            got_side.at[src, stages[s]],
            side_send.at[s, to],
            side_recv.at[s, src],
            rows=side * half + to,
        )

    def half_copy(s):
        return remote(
            half_sum.at[stages[s]],
            got_half.at[stages[s]],
            half_send.at[s],
            half_recv.at[s],
            rows=facing,
        )

    def total_copy(s, to, src):
        block = total.at[src, stages[s]]
        return remote(
            block, block, total_send.at[s, to], total_recv.at[s, src], rows=side * half + to
        )

    def sums_side(s):
        for k in range(1, half):
            side_copy(s, mate(k), member).start()

    def sums_across(s):
        acc = part[member, stages[s]]
        for k in range(1, half):
            side_copy(s, mate(k), mate(k)).wait_recv()
            acc = acc + got_side[mate(k), stages[s]]
        half_sum[stages[s]] = acc
        half_copy(s).start()

    def sums_back(s):
        half_copy(s).wait_recv()
        total[member, stages[s]] = half_sum[stages[s]] + got_half[stages[s]]
        for k in range(1, half):
            total_copy(s, mate(k), member).start()

    scales = (scale_gate, scale_up, scale_down)

    def sums_done(s):
        for k in range(1, half):
            total_copy(s, mate(k), mate(k)).wait_recv()
        for t in ((0,), (1, 2))[s]:
            for q in range(half):
                inverse[q, t] = 1.0 / (total[q, t] / count)
            mine = total[me // 2, t] / count
            scales[t][...] = jnp.where(lax.rem(me, 2) == 0, mine[:, :share], mine[:, share:])

    sums_side(0)

    def block_copy(t, g, to, src):
        start, size = groups[t][g]
        some = pl.ds(start, size)
        at = pl.ds(pl.multiple_of(src * rows, rows), rows)
        if t < 2:
            piece = send_wide.at[t, to, some]
            dst = (out_gate, out_up)[t].at[some, at, :]
        else:
            piece = send_tall.at[to, some]
            dst = out_down.at[some, :, at]
        b = base[t] + g
        return remote(piece, dst, bulk_send.at[b, to], bulk_recv.at[b, src], rows=to)

    def send_chip(t, g, there):
        for c in range(CORES):
            block_copy(t, g, there * CORES + lax.rem(core + c, CORES), me).start()

    def send_at(t, g, d):
        first_ones = t == 0 and g < early
        for way in (1, -1):
            there = chip + way * d
            ok = (there >= 0) & (there < chips)
            if first_ones:
                ok = ok & (there // half_chips == chip // half_chips)

            @pl.when(ok)
            def _():
                send_chip(t, g, there)

    def send_near(t, g):
        send_at(t, g, 1)
        for c in range(1, CORES):
            block_copy(t, g, chip * CORES + lax.rem(core + c, CORES), me).start()

    def send_across(g, k):
        there = jnp.where(side == 0, half_chips + k, half_chips - 1 - k)
        send_chip(0, g, there)

    def scaled_pair(t, e, q, block, factor):
        value = (block * factor).astype(jnp.bfloat16)
        for i in range(2):
            send_wide[t, 2 * q + i, e] = value[:, i * share : (i + 1) * share]

    def half_first(e, which, factor_of):
        for p in range(half // 2):
            q = which * (half // 2) + p
            at = pl.ds(pl.multiple_of(q * pair, pair), pair)
            scaled_pair(0, e, q, first[e, :, at], factor_of(p, q))

    def early_factor(e):
        return lambda p, q: early_inv[pl.ds(e, 1), p * pair : (p + 1) * pair]

    def ready_wide(t):
        def body(e, slot):
            for q in range(half):
                scaled_pair(
                    t,
                    e,
                    q,
                    wide[slot, :, q * pair : (q + 1) * pair],
                    inverse[q, t, pl.ds(e, 1), :],
                )

        return body

    def ready_tall(e, slot):
        for q in range(half):
            row = inverse[q, 2, pl.ds(e, 1), :]
            factor = jnp.broadcast_to(row, (128, pair)).T
            for c in range(0, rows, 128):
                block = tall[slot, q * pair : (q + 1) * pair, c : c + 128]
                value = (block * factor).astype(jnp.bfloat16)
                for i in range(2):
                    send_tall[2 * q + i, e, :, c : c + 128] = value[
                        i * share : (i + 1) * share
                    ]

    def own(t, start, stop):
        @pl.loop(start, stop)
        def _(e):
            if t < 2:
                (out_gate, out_up)[t][e, span, :] = send_wide[t, me, e]
            else:
                out_down[e, :, span] = send_tall[me, e]

    def ready(t, g, body):
        start, size = groups[t][g]
        run(t, start, start + size, body)

    acc = early_part[1 - side]
    for k in range(1, n):
        early_copy(peer(k), peer(k)).wait_recv()
        acc = acc + early_got[peer(k)]
    early_inv[...] = 1.0 / (acc / count)

    fill(1, 0)
    half_first(0, 1 - side, early_factor(0))
    send_across(0, 0)
    sums_across(0)
    for k in range(1, half_chips):
        send_across(0, k)
    for e in range(1, early):
        half_first(e, 1 - side, early_factor(e))
    run(1, 0, experts, sums_wide(1))
    fill(0, early)
    sums_back(0)
    for e in range(1, early):
        for k in range(half_chips):
            send_across(e, k)

    weight_load.wait()
    gain_load.wait()
    router[...] = (weight[...] * gain[...]).astype(jnp.bfloat16)
    out_router[home, :, span] = router[...]

    def strip(src):
        return out_router.at[home, :, pl.ds(pl.multiple_of(src * rows, rows), rows)]

    def router_copy(to, src):
        return remote(router, strip(src), router_send.at[to], router_recv.at[src], rows=to)

    def forward_copy(to, src):
        return remote(
            strip(lax.rem(src + half, n)),
            strip(lax.rem(src + half, n)),
            fwd_send.at[to],
            fwd_recv.at[src],
            rows=to,
        )

    def col_copy(to, src):
        return remote(
            out_router.at[src], out_router.at[src], col_send.at[to], col_recv.at[src], owner=to
        )

    for k in range(1, half):
        router_copy(side * half + mate(k), me).start()
    router_copy(facing, me).start()

    sums_done(0)

    for e in range(early):
        half_first(e, side, lambda p, q: inverse[q, 0, pl.ds(e, 1), :])
    for g in range(early):
        send_near(0, g)
    rest = range(early, len(groups[0]))
    for g in rest:
        ready(0, g, ready_wide(0))
        send_near(0, g)
    fill(2, 0)
    own(0, 0, experts)
    run(2, 0, experts, sums_tall)
    fill(1, 0)
    fill(2, 0)

    def spread(t, g, d):
        send_at(t, g, d)

    def two(g):
        if chips > 2:
            send_at(0, g, 2)

    cuts = [list(rest)[:1], list(rest)[1:2], list(rest)[2:]]
    sums_side(1)
    for g in range(early):
        two(g)
    for g in cuts[0]:
        two(g)
    sums_across(1)
    for g in cuts[1]:
        two(g)
    sums_back(1)
    for g in cuts[2]:
        two(g)

    router_copy(facing, facing).wait_recv()
    for k in range(1, half):
        forward_copy(side * half + mate(k), me).start()

    sums_done(1)
    for t, body in ((1, ready_wide(1)), (2, ready_tall)):
        for g in range(len(groups[t])):
            ready(t, g, body)
            send_near(t, g)
    for t in (1, 2):
        own(t, 0, experts)

    for k in range(1, half):
        other = side * half + mate(k)
        router_copy(other, other).wait_recv()
        forward_copy(other, other).wait_recv()
    for k in range(1, owners):
        col_copy(lax.rem(home + k, owners), home).start()

    for d in range(2, chips):
        for t in range(3):
            for g in range(len(groups[t])):
                if t == 0 and d == 2:
                    continue
                send_at(t, g, d)

    for k in range(1, owners):
        other = lax.rem(home + k, owners)
        col_copy(other, other).wait_recv()
        col_copy(other, home).wait_send()
    router_copy(facing, me).wait_send()
    for k in range(1, half):
        other = side * half + mate(k)
        router_copy(other, me).wait_send()
        forward_copy(other, me).wait_send()
        for s in range(2):
            side_copy(s, mate(k), member).wait_send()
            total_copy(s, mate(k), member).wait_send()
    for s in range(2):
        half_copy(s).wait_send()
    for k in range(1, n):
        early_copy(peer(k), me).wait_send()
    for t in range(3):
        for g in range(len(groups[t])):

            @pl.loop(1, n)
            def _(k):
                block_copy(t, g, peer(k), peer(k)).wait_recv()
                block_copy(t, g, peer(k), me).wait_send()


def write_back(count, *refs):
    ins, outs, sem = refs[:count], refs[count : 2 * count], refs[2 * count]
    copies = [
        pltpu.make_async_copy(a, b, sem.at[i]) for i, (a, b) in enumerate(zip(ins, outs))
    ]
    for copy in copies:
        copy.start()
    for copy in copies:
        copy.wait()


def local(n, owners, gate, up, down, router_weight, router_gain):
    experts, rows, width = gate.shape
    share = width // n
    half = n // 2
    pair = 2 * share
    early, groups, _, total_groups = plan(experts)
    slots = min(SLOTS, experts)
    router = router_weight.T
    gain = router_gain.reshape(1, -1)
    columns = router.shape[0]
    anywhere = pl.BlockSpec(memory_space=pl.ANY)
    vmem = pl.BlockSpec(memory_space=pltpu.VMEM)
    hbm = pl.BlockSpec(memory_space=pltpu.HBM)
    f32, bf16 = jnp.float32, jnp.bfloat16
    dma = pltpu.SemaphoreType.DMA
    shapes = (
        ((experts, rows * n, share), bf16),
        ((experts, rows * n, share), bf16),
        ((experts, share, rows * n), bf16),
        ((experts, share), f32),
        ((experts, share), f32),
        ((experts, share), f32),
        ((owners, columns, rows * n), bf16),
    )
    results = pl.pallas_call(
        functools.partial(exchange, n, owners),
        name="exchange",
        out_shape=tuple(pltpu.VMEM(*s) for s in shapes),
        in_specs=[anywhere] * 5,
        out_specs=(vmem,) * len(shapes),
        scratch_shapes=[
            pltpu.VMEM((early, rows, width), f32),
            pltpu.VMEM((slots, rows, width), f32),
            pltpu.VMEM((slots, width, rows), f32),
            pltpu.VMEM((2, n, experts, rows, share), bf16),
            pltpu.VMEM((n, experts, share, rows), bf16),
            pltpu.VMEM((2, early, width // 2), f32),
            pltpu.VMEM((n, early, width // 2), f32),
            pltpu.VMEM((early, width // 2), f32),
            pltpu.VMEM((half, 3, experts, pair), f32),
            pltpu.VMEM((half, 3, experts, pair), f32),
            pltpu.VMEM((3, experts, pair), f32),
            pltpu.VMEM((3, experts, pair), f32),
            pltpu.VMEM((half, 3, experts, pair), f32),
            pltpu.VMEM((half, 3, experts, pair), f32),
            pltpu.VMEM((columns, rows), f32),
            pltpu.VMEM((1, rows), f32),
            pltpu.VMEM((columns, rows), bf16),
            dma((4, max(slots, 2, early))),
            dma((n,)),
            dma((n,)),
            dma((2, half)),
            dma((2, half)),
            dma((2,)),
            dma((2,)),
            dma((2, half)),
            dma((2, half)),
            dma((n,)),
            dma((n,)),
            dma((n,)),
            dma((n,)),
            dma((owners,)),
            dma((owners,)),
            dma((total_groups, n)),
            dma((total_groups, n)),
        ],
        compiler_params=pltpu.CompilerParams(
            collective_id=0, has_side_effects=True, vmem_limit_bytes=38 * 1024 * 1024
        ),
    )(gate, up, down, router, gain)
    outs = pl.pallas_call(
        functools.partial(write_back, len(shapes)),
        name="write_back",
        out_shape=tuple(pltpu.HBM(*s) for s in shapes),
        in_specs=[vmem] * len(shapes),
        out_specs=(hbm,) * len(shapes),
        scratch_shapes=[dma((len(shapes),))],
        compiler_params=pltpu.CompilerParams(vmem_limit_bytes=1024 * 1024),
    )(*results)
    serve_router = outs[6].reshape(owners * columns, rows * n).T
    return (*outs[:6], serve_router)


def solution(mesh):
    return jax.shard_map(
        functools.partial(local, mesh.shape["rows"], mesh.shape["owner"]),
        mesh=mesh,
        in_specs=(
            P("owner", "rows", None),
            P("owner", "rows", None),
            P("owner", None, "rows"),
            P("rows", "owner"),
            P("rows"),
        ),
        out_specs=(
            P("owner", None, "rows"),
            P("owner", None, "rows"),
            P("owner", "rows", None),
            P("owner", "rows"),
            P("owner", "rows"),
            P("owner", "rows"),
            P(),
        ),
        check_vma=False,
    )
```

```python
import functools

import jax
import jax.numpy as jnp
from jax import lax
from jax.experimental import pallas as pl
from jax.experimental.pallas import tpu as pltpu
from jax.sharding import PartitionSpec as P

CORES = 2
SLOTS = 4
EARLY = 2
SHADOW = 6
CHUNKS = 4
GROUPS = 4
MESH = pl.DeviceIdType.MESH


def groups_of(experts, start):
    per = max(1, experts // GROUPS)
    out = [(e, 1) for e in range(start)]
    at = start
    while at < experts:
        end = min(experts, (at // per + 1) * per)
        out.append((at, end - at))
        at = end
    return out


def plan(experts):
    early = min(EARLY, experts // 2)
    groups = [groups_of(experts, early), groups_of(experts, 0), groups_of(experts, 0)]
    base = [0, len(groups[0]), len(groups[0]) + len(groups[1])]
    return early, groups, base, sum(len(g) for g in groups)


def exchange(
    n,
    owners,
    gate,
    up,
    down,
    router_weight,
    router_gain,
    out_gate,
    out_up,
    out_down,
    scale_gate,
    scale_up,
    scale_down,
    out_router,
    first,
    wide,
    tall,
    send_wide,
    send_tall,
    early_part,
    early_got,
    early_inv,
    part,
    got_side,
    half_sum,
    got_half,
    total,
    inverse,
    weight,
    gain,
    router,
    load_sem,
    early_send,
    early_recv,
    side_send,
    side_recv,
    half_send,
    half_recv,
    total_send,
    total_recv,
    router_send,
    router_recv,
    fwd_send,
    fwd_recv,
    col_send,
    col_recv,
    bulk_send,
    bulk_recv,
):
    me = lax.axis_index("rows")
    home = lax.axis_index("owner")
    experts, rows, width = gate.shape
    share = width // n
    pair = 2 * share
    half = n // 2
    slots = wide.shape[0]
    chips = n // CORES
    half_chips = chips // 2
    chip = me // CORES
    core = lax.rem(me, CORES)
    side = me // half
    member = lax.rem(me, half)
    facing = lax.rem(me + half, n)
    early, groups, base, _ = plan(experts)
    count = rows * n
    srcs = (gate, up, down)
    span = pl.ds(pl.multiple_of(me * rows, rows), rows)

    def peer(k):
        return lax.rem(me + k, n)

    def mate(k):
        return lax.rem(member + k, half)

    def remote(src, dst, out_sem, in_sem, **where):
        return pltpu.make_async_remote_copy(
            src_ref=src,
            dst_ref=dst,
            send_sem=out_sem,
            recv_sem=in_sem,
            device_id=where,
            device_id_type=MESH,
        )

    def load(t, e):
        buf = wide if t < 2 else tall
        slot = lax.rem(e, slots)
        return pltpu.make_async_copy(
            srcs[t].at[e], buf.at[slot], load_sem.at[0 if t < 2 else 1, slot]
        )

    def load_first(e):
        return pltpu.make_async_copy(gate.at[e], first.at[e], load_sem.at[2, e])

    for e in range(early):
        load_first(e).start()

    def fill(t, start, stop):
        for e in range(start, min(start + slots, stop)):
            load(t, e).start()

    def run(t, start, stop, last, body):
        @pl.loop(start, stop)
        def _(e):
            load(t, e).wait()
            body(e, lax.rem(e, slots))

            @pl.when(e + slots < last)
            def _():
                load(t, e + slots).start()

    fill(0, early, experts)
    weight_load = pltpu.make_async_copy(router_weight, weight, load_sem.at[3, 0])
    gain_load = pltpu.make_async_copy(router_gain, gain, load_sem.at[3, 1])
    weight_load.start()
    gain_load.start()

    barrier = pltpu.get_barrier_semaphore()
    for k in range(1, n):
        pl.semaphore_signal(barrier, inc=1, device_id={"rows": peer(k)}, device_id_type=MESH)
    for k in range(1, owners):
        pl.semaphore_signal(
            barrier, inc=1, device_id={"owner": lax.rem(home + k, owners)}, device_id_type=MESH
        )

    def put_part(t, e, sums):
        for q in range(half):
            part[q, t, pl.ds(e, 1), :] = sums[:, q * pair : (q + 1) * pair]

    def sums_wide(t):
        def body(e, slot):
            put_part(t, e, jnp.sum(jnp.abs(wide[slot]), axis=0, keepdims=True))

        return body

    def sums_tall(e, slot):
        for q in range(half):
            block = jnp.abs(tall[slot, q * pair : (q + 1) * pair, :])
            folded = block[:, :128]
            for c in range(128, rows, 128):
                folded = folded + block[:, c : c + 128]
            part[q, 2, pl.ds(e, 1), :] = jnp.sum(folded.T, axis=0, keepdims=True)

    for e in range(early):
        load_first(e).wait()
        sums = jnp.sum(jnp.abs(first[e]), axis=0, keepdims=True)
        put_part(0, e, sums)
        for s in range(2):
            early_part[s, pl.ds(e, 1), :] = sums[:, s * (width // 2) : (s + 1) * (width // 2)]

    pl.semaphore_wait(barrier, n - 1 + owners - 1)

    def early_copy(to, src):
        return remote(
            early_part.at[1 - to // half],
            early_got.at[src],
            early_send.at[to],
            early_recv.at[src],
            rows=to,
        )

    for k in range(1, n):
        early_copy(peer(k), me).start()

    weight_load.wait()
    gain_load.wait()
    router[...] = (weight[...] * gain[...]).astype(jnp.bfloat16)
    out_router[home, :, span] = router[...]

    def strip(src):
        return out_router.at[home, :, pl.ds(pl.multiple_of(src * rows, rows), rows)]

    def router_copy(to, src):
        return remote(router, strip(src), router_send.at[to], router_recv.at[src], rows=to)

    def forward_copy(to, src):
        return remote(
            strip(lax.rem(src + half, n)),
            strip(lax.rem(src + half, n)),
            fwd_send.at[to],
            fwd_recv.at[src],
            rows=to,
        )

    def col_copy(to, src):
        return remote(
            out_router.at[src], out_router.at[src], col_send.at[to], col_recv.at[src], owner=to
        )

    for k in range(1, half):
        router_copy(side * half + mate(k), me).start()
    router_copy(facing, me).start()

    shadow = min(early + SHADOW, experts)
    run(0, early, shadow, experts, sums_wide(0))

    stages = (pl.ds(0, 1), pl.ds(1, 2))

    def side_copy(s, to, src):
        return remote(
            part.at[to, stages[s]],
            got_side.at[src, stages[s]],
            side_send.at[s, to],
            side_recv.at[s, src],
            rows=side * half + to,
        )

    def half_copy(s):
        return remote(
            half_sum.at[stages[s]],
            got_half.at[stages[s]],
            half_send.at[s],
            half_recv.at[s],
            rows=facing,
        )

    def total_copy(s, to, src):
        block = total.at[src, stages[s]]
        return remote(
            block, block, total_send.at[s, to], total_recv.at[s, src], rows=side * half + to
        )

    def sums_side(s):
        for k in range(1, half):
            side_copy(s, mate(k), member).start()

    def sums_across(s):
        acc = part[member, stages[s]]
        for k in range(1, half):
            side_copy(s, mate(k), mate(k)).wait_recv()
            acc = acc + got_side[mate(k), stages[s]]
        half_sum[stages[s]] = acc
        half_copy(s).start()

    def sums_back(s):
        half_copy(s).wait_recv()
        total[member, stages[s]] = half_sum[stages[s]] + got_half[stages[s]]
        for k in range(1, half):
            total_copy(s, mate(k), member).start()

    scales = (scale_gate, scale_up, scale_down)

    def sums_done(s):
        for k in range(1, half):
            total_copy(s, mate(k), mate(k)).wait_recv()
        for t in ((0,), (1, 2))[s]:
            for q in range(half):
                inverse[q, t] = 1.0 / (total[q, t] / count)
            mine = total[me // 2, t] / count
            scales[t][...] = jnp.where(lax.rem(me, 2) == 0, mine[:, :share], mine[:, share:])

    def block_copy(t, g, to, src):
        start, size = groups[t][g]
        some = pl.ds(start, size)
        at = pl.ds(pl.multiple_of(src * rows, rows), rows)
        if t < 2:
            piece = send_wide.at[t, to, some]
            dst = (out_gate, out_up)[t].at[some, at, :]
        else:
            piece = send_tall.at[to, some]
            dst = out_down.at[some, :, at]
        b = base[t] + g
        return remote(piece, dst, bulk_send.at[b, to], bulk_recv.at[b, src], rows=to)

    def send_chip(t, g, there):
        for c in range(CORES):
            block_copy(t, g, there * CORES + lax.rem(core + c, CORES), me).start()

    def send_at(t, g, d):
        first_ones = t == 0 and g < early
        for way in (1, -1):
            there = chip + way * d
            ok = (there >= 0) & (there < chips)
            if first_ones:
                ok = ok & (there // half_chips == chip // half_chips)

            @pl.when(ok)
            def _():
                send_chip(t, g, there)

    def send_near(t, g):
        send_at(t, g, 1)
        for c in range(1, CORES):
            block_copy(t, g, chip * CORES + lax.rem(core + c, CORES), me).start()

    inner = (chip == half_chips - 1) | (chip == half_chips)

    def send_across(who, pieces):
        @pl.when(who)
        def _():
            for g, k in pieces:
                there = jnp.where(side == 0, half_chips + k, half_chips - 1 - k)
                send_chip(0, g, there)

    def scaled_pair(t, e, q, block, factor):
        value = (block * factor).astype(jnp.bfloat16)
        for i in range(2):
            send_wide[t, 2 * q + i, e] = value[:, i * share : (i + 1) * share]

    def half_first(e, which, factor_of):
        for p in range(half // 2):
            q = which * (half // 2) + p
            at = pl.ds(pl.multiple_of(q * pair, pair), pair)
            scaled_pair(0, e, q, first[e, :, at], factor_of(p, q))

    def early_factor(e):
        return lambda p, q: early_inv[pl.ds(e, 1), p * pair : (p + 1) * pair]

    def ready_wide(t):
        def body(e, slot):
            for q in range(half):
                scaled_pair(
                    t,
                    e,
                    q,
                    wide[slot, :, q * pair : (q + 1) * pair],
                    inverse[q, t, pl.ds(e, 1), :],
                )

        return body

    def ready_tall(e, slot):
        for q in range(half):
            row = inverse[q, 2, pl.ds(e, 1), :]
            factor = jnp.broadcast_to(row, (128, pair)).T
            for c in range(0, rows, 128):
                block = tall[slot, q * pair : (q + 1) * pair, c : c + 128]
                value = (block * factor).astype(jnp.bfloat16)
                for i in range(2):
                    send_tall[2 * q + i, e, :, c : c + 128] = value[
                        i * share : (i + 1) * share
                    ]

    def own(t, start, stop):
        @pl.loop(start, stop)
        def _(e):
            if t < 2:
                (out_gate, out_up)[t][e, span, :] = send_wide[t, me, e]
            else:
                out_down[e, :, span] = send_tall[me, e]

    def ready(t, g, last, body):
        start, size = groups[t][g]
        run(t, start, start + size, last, body)

    acc = early_part[1 - side]
    for k in range(1, n):
        early_copy(peer(k), peer(k)).wait_recv()
        acc = acc + early_got[peer(k)]
    early_inv[...] = 1.0 / (acc / count)

    pieces = [(e, k) for e in range(early) for k in range(half_chips)]
    cut = max(1, len(pieces) // 4)
    middle = experts // 2
    rest = range(early, len(groups[0]))
    low = [g for g in rest if groups[0][g][0] < middle]
    high = [g for g in rest if groups[0][g][0] >= middle]

    half_first(0, 1 - side, early_factor(0))
    send_across(inner, pieces[:cut])
    run(0, shadow, experts, experts, sums_wide(0))
    fill(1, 0, middle)
    sums_side(0)
    for e in range(1, early):
        half_first(e, 1 - side, early_factor(e))
    send_across(inner, pieces[cut : 2 * cut])
    sums_across(0)
    send_across(inner, pieces[2 * cut : 3 * cut])
    run(1, 0, middle, middle, sums_wide(1))
    fill(0, early, middle)
    fill(2, 0, experts)
    sums_back(0)
    send_across(inner, pieces[3 * cut :])
    send_across(jnp.logical_not(inner), pieces)
    sums_done(0)

    for g in low:
        ready(0, g, middle, ready_wide(0))
        send_near(0, g)
    fill(1, middle, experts)
    for e in range(early):
        half_first(e, side, lambda p, q: inverse[q, 0, pl.ds(e, 1), :])
    for g in range(early):
        send_near(0, g)
    run(1, middle, experts, experts, sums_wide(1))
    fill(0, middle, experts)
    run(2, 0, experts, experts, sums_tall)
    fill(2, 0, experts)
    sums_side(1)
    for g in high[:1]:
        ready(0, g, experts, ready_wide(0))
        send_near(0, g)
    sums_across(1)
    for g in high[1:]:
        ready(0, g, experts, ready_wide(0))
        send_near(0, g)
    fill(1, 0, experts)
    sums_back(1)

    def send_far(t, g):
        for d in range(2, chips):
            send_at(t, g, d)

    for g in low:
        send_far(0, g)
    own(0, 0, experts)
    router_copy(facing, facing).wait_recv()
    for k in range(1, half):
        forward_copy(side * half + mate(k), me).start()
    sums_done(1)
    for g in [*range(early), *high]:
        send_far(0, g)
    for t, body in ((1, ready_wide(1)), (2, ready_tall)):
        for g in range(len(groups[t])):
            ready(t, g, experts, body)
            send_far(t, g)
    for t in (1, 2):
        for g in range(len(groups[t])):
            send_near(t, g)
    for t in (1, 2):
        own(t, 0, experts)

    for k in range(1, half):
        other = side * half + mate(k)
        router_copy(other, other).wait_recv()
        forward_copy(other, other).wait_recv()
    for k in range(1, owners):
        col_copy(lax.rem(home + k, owners), home).start()

    for k in range(1, owners):
        other = lax.rem(home + k, owners)
        col_copy(other, other).wait_recv()
        col_copy(other, home).wait_send()
    router_copy(facing, me).wait_send()
    for k in range(1, half):
        other = side * half + mate(k)
        router_copy(other, me).wait_send()
        forward_copy(other, me).wait_send()
        for s in range(2):
            side_copy(s, mate(k), member).wait_send()
            total_copy(s, mate(k), member).wait_send()
    for s in range(2):
        half_copy(s).wait_send()
    for k in range(1, n):
        early_copy(peer(k), me).wait_send()
    for t in range(3):
        for g in range(len(groups[t])):

            @pl.loop(1, n)
            def _(k):
                block_copy(t, g, peer(k), peer(k)).wait_recv()
                block_copy(t, g, peer(k), me).wait_send()


def chunks_of(shape):
    count = CHUNKS if len(shape) == 3 and shape[0] % CHUNKS == 0 else 1
    size = shape[0] // count
    return [pl.ds(i * size, size) for i in range(count)]


def write_back(count, *refs):
    ins, outs, sem = refs[:count], refs[count : 2 * count], refs[2 * count]
    copies = []
    for i, (a, b) in enumerate(zip(ins, outs)):
        for j, some in enumerate(chunks_of(a.shape)):
            copies.append(pltpu.make_async_copy(a.at[some], b.at[some], sem.at[i, j]))
    for copy in copies:
        copy.start()
    for copy in copies:
        copy.wait()


def local(n, owners, gate, up, down, router_weight, router_gain):
    experts, rows, width = gate.shape
    share = width // n
    half = n // 2
    pair = 2 * share
    early, groups, _, total_groups = plan(experts)
    slots = min(SLOTS, experts)
    router = router_weight.T
    gain = router_gain.reshape(1, -1)
    columns = router.shape[0]
    anywhere = pl.BlockSpec(memory_space=pl.ANY)
    vmem = pl.BlockSpec(memory_space=pltpu.VMEM)
    hbm = pl.BlockSpec(memory_space=pltpu.HBM)
    f32, bf16 = jnp.float32, jnp.bfloat16
    dma = pltpu.SemaphoreType.DMA
    shapes = (
        ((experts, rows * n, share), bf16),
        ((experts, rows * n, share), bf16),
        ((experts, share, rows * n), bf16),
        ((experts, share), f32),
        ((experts, share), f32),
        ((experts, share), f32),
        ((owners, columns, rows * n), bf16),
    )
    results = pl.pallas_call(
        functools.partial(exchange, n, owners),
        name="exchange",
        out_shape=tuple(pltpu.VMEM(*s) for s in shapes),
        in_specs=[anywhere] * 5,
        out_specs=(vmem,) * len(shapes),
        scratch_shapes=[
            pltpu.VMEM((early, rows, width), f32),
            pltpu.VMEM((slots, rows, width), f32),
            pltpu.VMEM((slots, width, rows), f32),
            pltpu.VMEM((2, n, experts, rows, share), bf16),
            pltpu.VMEM((n, experts, share, rows), bf16),
            pltpu.VMEM((2, early, width // 2), f32),
            pltpu.VMEM((n, early, width // 2), f32),
            pltpu.VMEM((early, width // 2), f32),
            pltpu.VMEM((half, 3, experts, pair), f32),
            pltpu.VMEM((half, 3, experts, pair), f32),
            pltpu.VMEM((3, experts, pair), f32),
            pltpu.VMEM((3, experts, pair), f32),
            pltpu.VMEM((half, 3, experts, pair), f32),
            pltpu.VMEM((half, 3, experts, pair), f32),
            pltpu.VMEM((columns, rows), f32),
            pltpu.VMEM((1, rows), f32),
            pltpu.VMEM((columns, rows), bf16),
            dma((4, max(slots, 2, early))),
            dma((n,)),
            dma((n,)),
            dma((2, half)),
            dma((2, half)),
            dma((2,)),
            dma((2,)),
            dma((2, half)),
            dma((2, half)),
            dma((n,)),
            dma((n,)),
            dma((n,)),
            dma((n,)),
            dma((owners,)),
            dma((owners,)),
            dma((total_groups, n)),
            dma((total_groups, n)),
        ],
        compiler_params=pltpu.CompilerParams(
            collective_id=0, has_side_effects=True, vmem_limit_bytes=38 * 1024 * 1024
        ),
    )(gate, up, down, router, gain)
    outs = pl.pallas_call(
        functools.partial(write_back, len(shapes)),
        name="write_back",
        out_shape=tuple(pltpu.HBM(*s) for s in shapes),
        in_specs=[vmem] * len(shapes),
        out_specs=(hbm,) * len(shapes),
        scratch_shapes=[dma((len(shapes), CHUNKS))],
        compiler_params=pltpu.CompilerParams(vmem_limit_bytes=1024 * 1024),
    )(*results)
    serve_router = outs[6].reshape(owners * columns, rows * n).T
    return (*outs[:6], serve_router)


def solution(mesh):
    return jax.shard_map(
        functools.partial(local, mesh.shape["rows"], mesh.shape["owner"]),
        mesh=mesh,
        in_specs=(
            P("owner", "rows", None),
            P("owner", "rows", None),
            P("owner", None, "rows"),
            P("rows", "owner"),
            P("rows"),
        ),
        out_specs=(
            P("owner", None, "rows"),
            P("owner", None, "rows"),
            P("owner", "rows", None),
            P("owner", "rows"),
            P("owner", "rows"),
            P("owner", "rows"),
            P(),
        ),
        check_vma=False,
    )
```

```python
import functools

import jax
import jax.numpy as jnp
from jax import lax
from jax.experimental import pallas as pl
from jax.experimental.pallas import tpu as pltpu
from jax.sharding import PartitionSpec as P

CORES = 2
SLOTS = 4
EARLY = 2
SHADOW = 6
CHUNKS = 4
GROUPS = 4
MESH = pl.DeviceIdType.MESH


def groups_of(experts, start):
    per = max(1, experts // GROUPS)
    out = [(e, 1) for e in range(start)]
    at = start
    while at < experts:
        end = min(experts, (at // per + 1) * per)
        out.append((at, end - at))
        at = end
    return out


def plan(experts):
    early = min(EARLY, experts // 2)
    groups = [groups_of(experts, early), groups_of(experts, 0), groups_of(experts, 0)]
    base = [0, len(groups[0]), len(groups[0]) + len(groups[1])]
    return early, groups, base, sum(len(g) for g in groups)


def sides(n, me):
    chips = n // CORES
    chip = me // CORES
    inner = (chip == chips // 2 - 1) | (chip == chips // 2)
    return chip, inner, jnp.where(chip < chips // 2, chips // 2, chips // 2 - 1)


def exchange(
    n,
    owners,
    gate,
    up,
    down,
    router_weight,
    router_gain,
    out_gate,
    out_up,
    out_down,
    scale_gate,
    scale_up,
    scale_down,
    out_router,
    late_send,
    first,
    wide,
    tall,
    send_wide,
    send_tall,
    early_part,
    early_got,
    early_inv,
    part,
    got_side,
    half_sum,
    got_half,
    total,
    inverse,
    weight,
    gain,
    router,
    load_sem,
    early_send,
    early_recv,
    side_send,
    side_recv,
    half_send,
    half_recv,
    total_send,
    total_recv,
    router_send,
    router_recv,
    fwd_send,
    fwd_recv,
    col_send,
    col_recv,
    bulk_send,
    bulk_recv,
):
    me = lax.axis_index("rows")
    home = lax.axis_index("owner")
    experts, rows, width = gate.shape
    share = width // n
    pair = 2 * share
    half = n // 2
    slots = wide.shape[0]
    chips = n // CORES
    half_chips = chips // 2
    chip, inner, across = sides(n, me)
    core = lax.rem(me, CORES)
    side = me // half
    member = lax.rem(me, half)
    facing = lax.rem(me + half, n)
    early, groups, base, _ = plan(experts)
    count = rows * n
    srcs = (gate, up, down)
    span = pl.ds(pl.multiple_of(me * rows, rows), rows)

    def peer(k):
        return lax.rem(me + k, n)

    def mate(k):
        return lax.rem(member + k, half)

    def remote(src, dst, out_sem, in_sem, **where):
        return pltpu.make_async_remote_copy(
            src_ref=src,
            dst_ref=dst,
            send_sem=out_sem,
            recv_sem=in_sem,
            device_id=where,
            device_id_type=MESH,
        )

    def load(t, e):
        buf = wide if t < 2 else tall
        slot = lax.rem(e, slots)
        return pltpu.make_async_copy(
            srcs[t].at[e], buf.at[slot], load_sem.at[0 if t < 2 else 1, slot]
        )

    def load_first(e):
        return pltpu.make_async_copy(gate.at[e], first.at[e], load_sem.at[2, e])

    for e in range(early):
        load_first(e).start()

    def fill(t, start, stop):
        for e in range(start, min(start + slots, stop)):
            load(t, e).start()

    def run(t, start, stop, last, body):
        @pl.loop(start, stop)
        def _(e):
            load(t, e).wait()
            body(e, lax.rem(e, slots))

            @pl.when(e + slots < last)
            def _():
                load(t, e + slots).start()

    fill(0, early, experts)
    weight_load = pltpu.make_async_copy(router_weight, weight, load_sem.at[3, 0])
    gain_load = pltpu.make_async_copy(router_gain, gain, load_sem.at[3, 1])
    weight_load.start()
    gain_load.start()

    barrier = pltpu.get_barrier_semaphore()
    for k in range(1, n):
        pl.semaphore_signal(barrier, inc=1, device_id={"rows": peer(k)}, device_id_type=MESH)
    for k in range(1, owners):
        pl.semaphore_signal(
            barrier, inc=1, device_id={"owner": lax.rem(home + k, owners)}, device_id_type=MESH
        )

    def put_part(t, e, sums):
        for q in range(half):
            part[q, t, pl.ds(e, 1), :] = sums[:, q * pair : (q + 1) * pair]

    def sums_wide(t):
        def body(e, slot):
            put_part(t, e, jnp.sum(jnp.abs(wide[slot]), axis=0, keepdims=True))

        return body

    def sums_tall(e, slot):
        for q in range(half):
            block = jnp.abs(tall[slot, q * pair : (q + 1) * pair, :])
            folded = block[:, :128]
            for c in range(128, rows, 128):
                folded = folded + block[:, c : c + 128]
            part[q, 2, pl.ds(e, 1), :] = jnp.sum(folded.T, axis=0, keepdims=True)

    for e in range(early):
        load_first(e).wait()
        sums = jnp.sum(jnp.abs(first[e]), axis=0, keepdims=True)
        put_part(0, e, sums)
        for s in range(2):
            early_part[s, pl.ds(e, 1), :] = sums[:, s * (width // 2) : (s + 1) * (width // 2)]

    pl.semaphore_wait(barrier, n - 1 + owners - 1)

    def early_copy(to, src):
        return remote(
            early_part.at[1 - to // half],
            early_got.at[src],
            early_send.at[to],
            early_recv.at[src],
            rows=to,
        )

    for k in range(1, n):
        early_copy(peer(k), me).start()

    weight_load.wait()
    gain_load.wait()
    router[...] = (weight[...] * gain[...]).astype(jnp.bfloat16)
    out_router[home, :, span] = router[...]

    def strip(src):
        return out_router.at[home, :, pl.ds(pl.multiple_of(src * rows, rows), rows)]

    def router_copy(to, src):
        return remote(router, strip(src), router_send.at[to], router_recv.at[src], rows=to)

    def forward_copy(to, src):
        return remote(
            strip(lax.rem(src + half, n)),
            strip(lax.rem(src + half, n)),
            fwd_send.at[to],
            fwd_recv.at[src],
            rows=to,
        )

    def col_copy(to, src):
        return remote(
            out_router.at[src], out_router.at[src], col_send.at[to], col_recv.at[src], owner=to
        )

    for k in range(1, half):
        router_copy(side * half + mate(k), me).start()
    router_copy(facing, me).start()

    shadow = min(early + SHADOW, experts)
    run(0, early, shadow, experts, sums_wide(0))

    stages = (pl.ds(0, 1), pl.ds(1, 2))

    def side_copy(s, to, src):
        return remote(
            part.at[to, stages[s]],
            got_side.at[src, stages[s]],
            side_send.at[s, to],
            side_recv.at[s, src],
            rows=side * half + to,
        )

    def half_copy(s):
        return remote(
            half_sum.at[stages[s]],
            got_half.at[stages[s]],
            half_send.at[s],
            half_recv.at[s],
            rows=facing,
        )

    def total_copy(s, to, src):
        block = total.at[src, stages[s]]
        return remote(
            block, block, total_send.at[s, to], total_recv.at[s, src], rows=side * half + to
        )

    def sums_side(s):
        for k in range(1, half):
            side_copy(s, mate(k), member).start()

    def sums_across(s):
        acc = part[member, stages[s]]
        for k in range(1, half):
            side_copy(s, mate(k), mate(k)).wait_recv()
            acc = acc + got_side[mate(k), stages[s]]
        half_sum[stages[s]] = acc
        half_copy(s).start()

    def sums_back(s):
        half_copy(s).wait_recv()
        total[member, stages[s]] = half_sum[stages[s]] + got_half[stages[s]]
        for k in range(1, half):
            total_copy(s, mate(k), member).start()

    scales = (scale_gate, scale_up, scale_down)

    def sums_done(s):
        for k in range(1, half):
            total_copy(s, mate(k), mate(k)).wait_recv()
        for t in ((0,), (1, 2))[s]:
            for q in range(half):
                inverse[q, t] = 1.0 / (total[q, t] / count)
            mine = total[me // 2, t] / count
            scales[t][...] = jnp.where(lax.rem(me, 2) == 0, mine[:, :share], mine[:, share:])

    def block_copy(t, g, to, src):
        start, size = groups[t][g]
        some = pl.ds(start, size)
        at = pl.ds(pl.multiple_of(src * rows, rows), rows)
        if t < 2:
            piece = send_wide.at[t, to, some]
            dst = (out_gate, out_up)[t].at[some, at, :]
        else:
            piece = send_tall.at[to, some]
            dst = out_down.at[some, :, at]
        b = base[t] + g
        return remote(piece, dst, bulk_send.at[b, to], bulk_recv.at[b, src], rows=to)

    def send_chip(t, g, there):
        for c in range(CORES):
            block_copy(t, g, there * CORES + lax.rem(core + c, CORES), me).start()

    def send_side(t, g):
        for d in range(1, half_chips):
            for way in (1, -1):
                there = chip + way * d

                @pl.when((there // half_chips == chip // half_chips) & (there >= 0))
                def _():
                    send_chip(t, g, there)

        for c in range(1, CORES):
            block_copy(t, g, chip * CORES + lax.rem(core + c, CORES), me).start()

    last = (2, len(groups[2]) - 1)

    def send_across(who, pieces):
        @pl.when(who)
        def _():
            for t, g, k in pieces:
                there = jnp.where(side == 0, half_chips + k, half_chips - 1 - k)
                send_chip(t, g, there)

    def scaled_pair(t, e, q, block, factor):
        value = (block * factor).astype(jnp.bfloat16)
        for i in range(2):
            send_wide[t, 2 * q + i, e] = value[:, i * share : (i + 1) * share]

    def half_first(e, which, factor_of):
        for p in range(half // 2):
            q = which * (half // 2) + p
            at = pl.ds(pl.multiple_of(q * pair, pair), pair)
            scaled_pair(0, e, q, first[e, :, at], factor_of(p, q))

    def early_factor(e):
        return lambda p, q: early_inv[pl.ds(e, 1), p * pair : (p + 1) * pair]

    def ready_wide(t):
        def body(e, slot):
            for q in range(half):
                scaled_pair(
                    t,
                    e,
                    q,
                    wide[slot, :, q * pair : (q + 1) * pair],
                    inverse[q, t, pl.ds(e, 1), :],
                )

        return body

    def ready_tall(e, slot):
        for q in range(half):
            row = inverse[q, 2, pl.ds(e, 1), :]
            factor = jnp.broadcast_to(row, (128, pair)).T
            for c in range(0, rows, 128):
                block = tall[slot, q * pair : (q + 1) * pair, c : c + 128]
                value = (block * factor).astype(jnp.bfloat16)
                for i in range(2):
                    send_tall[2 * q + i, e, :, c : c + 128] = value[
                        i * share : (i + 1) * share
                    ]

    def own(t, start, stop):
        @pl.loop(start, stop)
        def _(e):
            if t < 2:
                (out_gate, out_up)[t][e, span, :] = send_wide[t, me, e]
            else:
                out_down[e, :, span] = send_tall[me, e]

    def ready(t, g, last, body):
        start, size = groups[t][g]
        run(t, start, start + size, last, body)

    acc = early_part[1 - side]
    for k in range(1, n):
        early_copy(peer(k), peer(k)).wait_recv()
        acc = acc + early_got[peer(k)]
    early_inv[...] = 1.0 / (acc / count)

    pieces = [(0, e, k) for e in range(early) for k in range(half_chips)]
    outer = jnp.logical_not(inner)
    cut = max(1, len(pieces) // 4)
    middle = experts // 2
    rest = range(early, len(groups[0]))
    low = [g for g in rest if groups[0][g][0] < middle]
    high = [g for g in rest if groups[0][g][0] >= middle]

    half_first(0, 1 - side, early_factor(0))
    send_across(inner, pieces[:cut])
    run(0, shadow, experts, experts, sums_wide(0))
    fill(1, 0, middle)
    sums_side(0)
    for e in range(1, early):
        half_first(e, 1 - side, early_factor(e))
    send_across(inner, pieces[cut : 2 * cut])
    sums_across(0)
    send_across(inner, pieces[2 * cut : 3 * cut])
    run(1, 0, middle, middle, sums_wide(1))
    fill(0, early, middle)
    fill(2, 0, experts)
    sums_back(0)
    send_across(inner, pieces[3 * cut :])
    send_across(outer, pieces)
    sums_done(0)

    def next_group(g, stop):
        ready(0, g, stop, ready_wide(0))
        send_across(inner, [(0, g, 0)])
        send_side(0, g)

    for g in low:
        next_group(g, middle)
    fill(1, middle, experts)
    for e in range(early):
        half_first(e, side, lambda p, q: inverse[q, 0, pl.ds(e, 1), :])
    for g in range(early):
        send_side(0, g)
    run(1, middle, experts, experts, sums_wide(1))
    fill(0, middle, experts)
    run(2, 0, experts, experts, sums_tall)
    fill(2, 0, experts)
    sums_side(1)
    for g in high[:1]:
        next_group(g, experts)
    sums_across(1)
    for g in high[1:]:
        next_group(g, experts)
    fill(1, 0, experts)
    sums_back(1)
    send_across(inner, [(0, g, k) for g in low for k in range(1, half_chips)])
    own(0, 0, experts)
    router_copy(facing, facing).wait_recv()
    for k in range(1, half):
        forward_copy(side * half + mate(k), me).start()
    sums_done(1)
    send_across(inner, [(0, g, k) for g in high for k in range(1, half_chips)])
    for t, body in ((1, ready_wide(1)), (2, ready_tall)):
        for g in range(len(groups[t])):
            ready(t, g, experts, body)
            send_across(inner, [(t, g, k) for k in range(half_chips) if (t, g, k) != (*last, 0)])
            send_side(t, g)
    start, size = groups[2][-1]
    for c in range(CORES):
        late_send[c] = send_tall[across * CORES + c, pl.ds(start, size)]
    for t in (1, 2):
        own(t, 0, experts)

    for k in range(1, half):
        other = side * half + mate(k)
        router_copy(other, other).wait_recv()
        forward_copy(other, other).wait_recv()
    for k in range(1, owners):
        col_copy(lax.rem(home + k, owners), home).start()

    @pl.when(outer)
    def _():
        for c in range(CORES):
            block_copy(*last, across * CORES + c, across * CORES + c).wait_recv()

    for k in range(half_chips):
        send_across(
            outer,
            [
                (t, g, k)
                for t in range(3)
                for g in range(early if t == 0 else 0, len(groups[t]))
            ],
        )

    for k in range(1, owners):
        other = lax.rem(home + k, owners)
        col_copy(other, other).wait_recv()
        col_copy(other, home).wait_send()
    router_copy(facing, me).wait_send()
    for k in range(1, half):
        other = side * half + mate(k)
        router_copy(other, me).wait_send()
        forward_copy(other, me).wait_send()
        for s in range(2):
            side_copy(s, mate(k), member).wait_send()
            total_copy(s, mate(k), member).wait_send()
    for s in range(2):
        half_copy(s).wait_send()
    for k in range(1, n):
        early_copy(peer(k), me).wait_send()
    for t in range(3):
        for g in range(len(groups[t])):

            @pl.loop(1, n)
            def _(k):
                other = peer(k)
                if (t, g) != last:
                    block_copy(t, g, other, other).wait_recv()
                    block_copy(t, g, other, me).wait_send()
                else:
                    facing_chip = other // CORES == across

                    @pl.when(jnp.logical_not(facing_chip))
                    def _():
                        block_copy(t, g, other, other).wait_recv()

                    @pl.when(jnp.logical_not(facing_chip & inner))
                    def _():
                        block_copy(t, g, other, me).wait_send()


def late_exchange(n, late_send, _, late_got, send_sem, recv_sem):
    me = lax.axis_index("rows")
    _, inner, across = sides(n, me)
    core = lax.rem(me, CORES)

    def copy(to, src):
        return pltpu.make_async_remote_copy(
            src_ref=late_send.at[to],
            dst_ref=late_got.at[src],
            send_sem=send_sem.at[to],
            recv_sem=recv_sem.at[src],
            device_id={"rows": across * CORES + to},
            device_id_type=MESH,
        )

    @pl.when(inner)
    def _():
        barrier = pltpu.get_barrier_semaphore()
        for c in range(CORES):
            pl.semaphore_signal(
                barrier, inc=1, device_id={"rows": across * CORES + c}, device_id_type=MESH
            )
        pl.semaphore_wait(barrier, CORES)
        for c in range(CORES):
            copy(lax.rem(core + c, CORES), core).start()
        for c in range(CORES):
            copy(c, c).wait_recv()
            copy(c, core).wait_send()


def late_place(n, start, late_got, down, out, sem):
    me = lax.axis_index("rows")
    _, inner, across = sides(n, me)
    size, rows = late_got.shape[1], late_got.shape[3]

    @pl.when(inner)
    def _():
        copies = []
        for c in range(CORES):
            src = across * CORES + c
            at = pl.ds(pl.multiple_of(src * rows, rows), rows)
            copies.append(
                pltpu.make_async_copy(
                    late_got.at[c], out.at[pl.ds(start, size), :, at], sem.at[c]
                )
            )
        for copy in copies:
            copy.start()
        for copy in copies:
            copy.wait()


def chunks_of(shape):
    count = CHUNKS if len(shape) == 3 and shape[0] % CHUNKS == 0 else 1
    size = shape[0] // count
    return [pl.ds(i * size, size) for i in range(count)]


def write_back(count, *refs):
    ins, outs, sem = refs[:count], refs[count : 2 * count], refs[2 * count]
    copies = []
    for i, (a, b) in enumerate(zip(ins, outs)):
        for j, some in enumerate(chunks_of(a.shape)):
            copies.append(pltpu.make_async_copy(a.at[some], b.at[some], sem.at[i, j]))
    for copy in copies:
        copy.start()
    for copy in copies:
        copy.wait()


def local(n, owners, gate, up, down, router_weight, router_gain):
    experts, rows, width = gate.shape
    share = width // n
    half = n // 2
    pair = 2 * share
    early, groups, _, total_groups = plan(experts)
    slots = min(SLOTS, experts)
    router = router_weight.T
    gain = router_gain.reshape(1, -1)
    columns = router.shape[0]
    anywhere = pl.BlockSpec(memory_space=pl.ANY)
    vmem = pl.BlockSpec(memory_space=pltpu.VMEM)
    hbm = pl.BlockSpec(memory_space=pltpu.HBM)
    f32, bf16 = jnp.float32, jnp.bfloat16
    dma = pltpu.SemaphoreType.DMA
    shapes = (
        ((experts, rows * n, share), bf16),
        ((experts, rows * n, share), bf16),
        ((experts, share, rows * n), bf16),
        ((experts, share), f32),
        ((experts, share), f32),
        ((experts, share), f32),
        ((owners, columns, rows * n), bf16),
    )
    start, size = groups[2][-1]
    late = ((CORES, size, share, rows), bf16)
    *results, late_send = pl.pallas_call(
        functools.partial(exchange, n, owners),
        name="exchange",
        out_shape=tuple(pltpu.VMEM(*s) for s in (*shapes, late)),
        in_specs=[anywhere] * 5,
        out_specs=(vmem,) * (len(shapes) + 1),
        scratch_shapes=[
            pltpu.VMEM((early, rows, width), f32),
            pltpu.VMEM((slots, rows, width), f32),
            pltpu.VMEM((slots, width, rows), f32),
            pltpu.VMEM((2, n, experts, rows, share), bf16),
            pltpu.VMEM((n, experts, share, rows), bf16),
            pltpu.VMEM((2, early, width // 2), f32),
            pltpu.VMEM((n, early, width // 2), f32),
            pltpu.VMEM((early, width // 2), f32),
            pltpu.VMEM((half, 3, experts, pair), f32),
            pltpu.VMEM((half, 3, experts, pair), f32),
            pltpu.VMEM((3, experts, pair), f32),
            pltpu.VMEM((3, experts, pair), f32),
            pltpu.VMEM((half, 3, experts, pair), f32),
            pltpu.VMEM((half, 3, experts, pair), f32),
            pltpu.VMEM((columns, rows), f32),
            pltpu.VMEM((1, rows), f32),
            pltpu.VMEM((columns, rows), bf16),
            dma((4, max(slots, 2, early))),
            dma((n,)),
            dma((n,)),
            dma((2, half)),
            dma((2, half)),
            dma((2,)),
            dma((2,)),
            dma((2, half)),
            dma((2, half)),
            dma((n,)),
            dma((n,)),
            dma((n,)),
            dma((n,)),
            dma((owners,)),
            dma((owners,)),
            dma((total_groups, n)),
            dma((total_groups, n)),
        ],
        compiler_params=pltpu.CompilerParams(
            collective_id=0, has_side_effects=True, vmem_limit_bytes=38 * 1024 * 1024
        ),
    )(gate, up, down, router, gain)
    outs = pl.pallas_call(
        functools.partial(write_back, len(shapes)),
        name="write_back",
        out_shape=tuple(pltpu.HBM(*s) for s in shapes),
        in_specs=[vmem] * len(shapes),
        out_specs=(hbm,) * len(shapes),
        scratch_shapes=[dma((len(shapes), CHUNKS))],
        compiler_params=pltpu.CompilerParams(vmem_limit_bytes=1024 * 1024),
    )(*results)
    late_got = pl.pallas_call(
        functools.partial(late_exchange, n),
        name="late_exchange",
        out_shape=pltpu.VMEM(*late),
        in_specs=[vmem, anywhere],
        out_specs=vmem,
        scratch_shapes=[dma((CORES,)), dma((CORES,))],
        compiler_params=pltpu.CompilerParams(
            collective_id=1, has_side_effects=True, vmem_limit_bytes=1024 * 1024
        ),
    )(late_send, outs[3])
    ready_down = pl.pallas_call(
        functools.partial(late_place, n, start),
        name="late_place",
        out_shape=pltpu.HBM(*shapes[2]),
        in_specs=[vmem, hbm],
        out_specs=hbm,
        scratch_shapes=[dma((CORES,))],
        input_output_aliases={1: 0},
        compiler_params=pltpu.CompilerParams(vmem_limit_bytes=1024 * 1024),
    )(late_got, outs[2])
    serve_router = outs[6].reshape(owners * columns, rows * n).T
    return (*outs[:2], ready_down, *outs[3:6], serve_router)


def solution(mesh):
    return jax.shard_map(
        functools.partial(local, mesh.shape["rows"], mesh.shape["owner"]),
        mesh=mesh,
        in_specs=(
            P("owner", "rows", None),
            P("owner", "rows", None),
            P("owner", None, "rows"),
            P("rows", "owner"),
            P("rows"),
        ),
        out_specs=(
            P("owner", None, "rows"),
            P("owner", None, "rows"),
            P("owner", "rows", None),
            P("owner", "rows"),
            P("owner", "rows"),
            P("owner", "rows"),
            P(),
        ),
        check_vma=False,
    )
```

```python
import functools

import jax
import jax.numpy as jnp
from jax import lax
from jax.experimental import pallas as pl
from jax.experimental.pallas import tpu as pltpu
from jax.sharding import PartitionSpec as P

CORES = 2
SLOTS = 4
EARLY = 3
SHADOW = 6
CHUNKS = 4
GROUPS = 4
MESH = pl.DeviceIdType.MESH


def groups_of(experts, start):
    per = max(1, experts // GROUPS)
    out = [(e, 1) for e in range(start)]
    at = start
    while at < experts:
        end = min(experts, (at // per + 1) * per)
        out.append((at, end - at))
        at = end
    return out


def plan(experts):
    early = max(1, min(EARLY, experts // 4))
    groups = [groups_of(experts, early), groups_of(experts, 0), groups_of(experts, 0)]
    (start, size), (_, more) = groups[2][-2:]
    groups[2][-2:] = [(start, size + more)]
    base = [0, len(groups[0]), len(groups[0]) + len(groups[1])]
    return early, groups, base, sum(len(g) for g in groups)


def sides(n, me):
    chips = n // CORES
    chip = me // CORES
    inner = (chip == chips // 2 - 1) | (chip == chips // 2)
    return chip, inner, jnp.where(chip < chips // 2, chips // 2, chips // 2 - 1)


def exchange(
    n,
    owners,
    gate,
    up,
    down,
    router_weight,
    router_gain,
    out_gate,
    out_up,
    out_down,
    scale_gate,
    scale_up,
    scale_down,
    out_router,
    late_send,
    first,
    wide,
    tall,
    send_wide,
    send_tall,
    early_part,
    early_got,
    early_inv,
    part,
    got_side,
    half_sum,
    got_half,
    total,
    inverse,
    weight,
    gain,
    router,
    load_sem,
    early_send,
    early_recv,
    side_send,
    side_recv,
    half_send,
    half_recv,
    total_send,
    total_recv,
    router_send,
    router_recv,
    fwd_send,
    fwd_recv,
    col_send,
    col_recv,
    bulk_send,
    bulk_recv,
):
    me = lax.axis_index("rows")
    home = lax.axis_index("owner")
    experts, rows, width = gate.shape
    share = width // n
    pair = 2 * share
    half = n // 2
    slots = wide.shape[0]
    chips = n // CORES
    half_chips = chips // 2
    chip, inner, across = sides(n, me)
    core = lax.rem(me, CORES)
    side = me // half
    member = lax.rem(me, half)
    facing = lax.rem(me + half, n)
    early, groups, base, _ = plan(experts)
    count = rows * n
    srcs = (gate, up, down)
    span = pl.ds(pl.multiple_of(me * rows, rows), rows)

    def peer(k):
        return lax.rem(me + k, n)

    def mate(k):
        return lax.rem(member + k, half)

    def remote(src, dst, out_sem, in_sem, **where):
        return pltpu.make_async_remote_copy(
            src_ref=src,
            dst_ref=dst,
            send_sem=out_sem,
            recv_sem=in_sem,
            device_id=where,
            device_id_type=MESH,
        )

    def load(t, e):
        buf = wide if t < 2 else tall
        slot = lax.rem(e, slots)
        return pltpu.make_async_copy(
            srcs[t].at[e], buf.at[slot], load_sem.at[0 if t < 2 else 1, slot]
        )

    def load_first(e):
        return pltpu.make_async_copy(gate.at[e], first.at[e], load_sem.at[2, e])

    for e in range(early):
        load_first(e).start()

    def fill(t, start, stop):
        for e in range(start, min(start + slots, stop)):
            load(t, e).start()

    def run(t, start, stop, last, body):
        @pl.loop(start, stop)
        def _(e):
            load(t, e).wait()
            body(e, lax.rem(e, slots))

            @pl.when(e + slots < last)
            def _():
                load(t, e + slots).start()

    fill(0, early, experts)
    weight_load = pltpu.make_async_copy(router_weight, weight, load_sem.at[3, 0])
    gain_load = pltpu.make_async_copy(router_gain, gain, load_sem.at[3, 1])
    weight_load.start()
    gain_load.start()

    barrier = pltpu.get_barrier_semaphore()
    for k in range(1, n):
        pl.semaphore_signal(barrier, inc=1, device_id={"rows": peer(k)}, device_id_type=MESH)
    for k in range(1, owners):
        pl.semaphore_signal(
            barrier, inc=1, device_id={"owner": lax.rem(home + k, owners)}, device_id_type=MESH
        )

    def put_part(t, e, sums):
        for q in range(half):
            part[q, t, pl.ds(e, 1), :] = sums[:, q * pair : (q + 1) * pair]

    def sums_wide(t):
        def body(e, slot):
            put_part(t, e, jnp.sum(jnp.abs(wide[slot]), axis=0, keepdims=True))

        return body

    def sums_tall(e, slot):
        for q in range(half):
            block = jnp.abs(tall[slot, q * pair : (q + 1) * pair, :])
            folded = block[:, :128]
            for c in range(128, rows, 128):
                folded = folded + block[:, c : c + 128]
            part[q, 2, pl.ds(e, 1), :] = jnp.sum(folded.T, axis=0, keepdims=True)

    for e in range(early):
        load_first(e).wait()
        sums = jnp.sum(jnp.abs(first[e]), axis=0, keepdims=True)
        put_part(0, e, sums)
        for s in range(2):
            early_part[s, pl.ds(e, 1), :] = sums[:, s * (width // 2) : (s + 1) * (width // 2)]

    pl.semaphore_wait(barrier, n - 1 + owners - 1)

    inners = (half_chips - 1, half_chips)
    reach = [c * CORES + i for c in inners for i in range(CORES)]

    def early_copy(to, src):
        return remote(
            early_part.at[1 - to // half],
            early_got.at[src],
            early_send.at[to],
            early_recv.at[src],
            rows=to,
        )

    for to in reach:

        @pl.when(me != to)
        def _():
            early_copy(to, me).start()

    weight_load.wait()
    gain_load.wait()
    router[...] = (weight[...] * gain[...]).astype(jnp.bfloat16)
    out_router[home, :, span] = router[...]

    def strip(src):
        return out_router.at[home, :, pl.ds(pl.multiple_of(src * rows, rows), rows)]

    def router_copy(to, src):
        return remote(router, strip(src), router_send.at[to], router_recv.at[src], rows=to)

    def forward_copy(to, src):
        return remote(
            strip(lax.rem(src + half, n)),
            strip(lax.rem(src + half, n)),
            fwd_send.at[to],
            fwd_recv.at[src],
            rows=to,
        )

    def col_copy(to, src):
        return remote(
            out_router.at[src], out_router.at[src], col_send.at[to], col_recv.at[src], owner=to
        )

    for k in range(1, half):
        router_copy(side * half + mate(k), me).start()
    router_copy(facing, me).start()

    shadow = min(early + SHADOW, experts)
    run(0, early, shadow, experts, sums_wide(0))

    stages = (pl.ds(0, 1), pl.ds(1, 2))

    def side_copy(s, to, src):
        return remote(
            part.at[to, stages[s]],
            got_side.at[src, stages[s]],
            side_send.at[s, to],
            side_recv.at[s, src],
            rows=side * half + to,
        )

    def half_copy(s):
        return remote(
            half_sum.at[stages[s]],
            got_half.at[stages[s]],
            half_send.at[s],
            half_recv.at[s],
            rows=facing,
        )

    def total_copy(s, to, src):
        block = total.at[src, stages[s]]
        return remote(
            block, block, total_send.at[s, to], total_recv.at[s, src], rows=side * half + to
        )

    def sums_side(s):
        for k in range(1, half):
            side_copy(s, mate(k), member).start()

    def sums_across(s):
        acc = part[member, stages[s]]
        for k in range(1, half):
            side_copy(s, mate(k), mate(k)).wait_recv()
            acc = acc + got_side[mate(k), stages[s]]
        half_sum[stages[s]] = acc
        half_copy(s).start()

    def sums_back(s):
        half_copy(s).wait_recv()
        total[member, stages[s]] = half_sum[stages[s]] + got_half[stages[s]]
        for k in range(1, half):
            total_copy(s, mate(k), member).start()

    scales = (scale_gate, scale_up, scale_down)

    def sums_done(s):
        for k in range(1, half):
            total_copy(s, mate(k), mate(k)).wait_recv()
        for t in ((0,), (1, 2))[s]:
            for q in range(half):
                inverse[q, t] = 1.0 / (total[q, t] / count)
            mine = total[me // 2, t] / count
            scales[t][...] = jnp.where(lax.rem(me, 2) == 0, mine[:, :share], mine[:, share:])

    def block_copy(t, g, to, src):
        start, size = groups[t][g]
        some = pl.ds(start, size)
        at = pl.ds(pl.multiple_of(src * rows, rows), rows)
        if t < 2:
            piece = send_wide.at[t, to, some]
            dst = (out_gate, out_up)[t].at[some, at, :]
        else:
            piece = send_tall.at[to, some]
            dst = out_down.at[some, :, at]
        b = base[t] + g
        return remote(piece, dst, bulk_send.at[b, to], bulk_recv.at[b, src], rows=to)

    def send_chip(t, g, there):
        for c in range(CORES):
            block_copy(t, g, there * CORES + lax.rem(core + c, CORES), me).start()

    def send_side(t, g):
        for d in range(1, half_chips):
            for way in (1, -1):
                there = chip + way * d

                @pl.when((there // half_chips == chip // half_chips) & (there >= 0))
                def _():
                    send_chip(t, g, there)

        for c in range(1, CORES):
            block_copy(t, g, chip * CORES + lax.rem(core + c, CORES), me).start()

    last = (2, len(groups[2]) - 1)
    held, want = [], groups[2][-1][1] - 1
    for g in reversed(range(len(groups[0]))):
        if groups[0][g][1] <= want:
            held.append(g)
            want -= groups[0][g][1]

    def send_across(who, pieces):
        @pl.when(who)
        def _():
            for t, g, k in pieces:
                there = jnp.where(side == 0, half_chips + k, half_chips - 1 - k)
                send_chip(t, g, there)

    def scaled_pair(t, e, q, block, factor):
        value = (block * factor).astype(jnp.bfloat16)
        for i in range(2):
            send_wide[t, 2 * q + i, e] = value[:, i * share : (i + 1) * share]

    def half_first(e, which, factor_of):
        for p in range(half // 2):
            q = which * (half // 2) + p
            at = pl.ds(pl.multiple_of(q * pair, pair), pair)
            scaled_pair(0, e, q, first[e, :, at], factor_of(p, q))

    def early_factor(e):
        return lambda p, q: early_inv[pl.ds(e, 1), p * pair : (p + 1) * pair]

    def late_factor(e):
        return lambda p, q: inverse[q, 0, pl.ds(e, 1), :]

    def ready_wide(t):
        def body(e, slot):
            for q in range(half):
                scaled_pair(
                    t,
                    e,
                    q,
                    wide[slot, :, q * pair : (q + 1) * pair],
                    inverse[q, t, pl.ds(e, 1), :],
                )

        return body

    def ready_tall(e, slot):
        for q in range(half):
            row = inverse[q, 2, pl.ds(e, 1), :]
            factor = jnp.broadcast_to(row, (128, pair)).T
            for c in range(0, rows, 128):
                block = tall[slot, q * pair : (q + 1) * pair, c : c + 128]
                value = (block * factor).astype(jnp.bfloat16)
                for i in range(2):
                    send_tall[2 * q + i, e, :, c : c + 128] = value[
                        i * share : (i + 1) * share
                    ]

    def own(t, start, stop):
        @pl.loop(start, stop)
        def _(e):
            if t < 2:
                (out_gate, out_up)[t][e, span, :] = send_wide[t, me, e]
            else:
                out_down[e, :, span] = send_tall[me, e]

    def ready(t, g, last, body):
        start, size = groups[t][g]
        run(t, start, start + size, last, body)

    @pl.when(inner)
    def _():
        acc = early_part[1 - side]
        for k in range(1, n):
            early_copy(peer(k), peer(k)).wait_recv()
            acc = acc + early_got[peer(k)]
        early_inv[...] = 1.0 / (acc / count)

    pieces = [(0, e, k) for e in range(early) for k in range(half_chips)]
    outer = jnp.logical_not(inner)
    cut = max(1, len(pieces) // 4)
    middle = experts // 2
    rest = range(early, len(groups[0]))
    low = [g for g in rest if groups[0][g][0] < middle]
    high = [g for g in rest if groups[0][g][0] >= middle]

    def early_ready(e):
        @pl.when(inner)
        def _():
            half_first(e, 1 - side, early_factor(e))

    early_ready(0)
    send_across(inner, pieces[:cut])
    run(0, shadow, experts, experts, sums_wide(0))
    fill(1, 0, middle)
    sums_side(0)
    for e in range(1, early):
        early_ready(e)
    send_across(inner, pieces[cut : 2 * cut])
    sums_across(0)
    send_across(inner, pieces[2 * cut : 3 * cut])
    run(1, 0, middle, middle, sums_wide(1))
    fill(0, early, middle)
    fill(2, 0, experts)
    sums_back(0)
    send_across(inner, pieces[3 * cut :])
    sums_done(0)

    def send_gate_side(g):
        if g in held:

            @pl.when(inner)
            def _():
                send_side(0, g)
        else:
            send_side(0, g)

    def next_group(g, stop):
        ready(0, g, stop, ready_wide(0))
        send_across(inner, [(0, g, 0)])
        send_gate_side(g)

    for g in low:
        next_group(g, middle)
    fill(1, middle, experts)
    for e in range(early):
        half_first(e, side, late_factor(e))

        @pl.when(outer)
        def _():
            half_first(e, 1 - side, late_factor(e))

    for g in range(early):
        send_gate_side(g)
    run(1, middle, experts, experts, sums_wide(1))
    fill(0, middle, experts)
    run(2, 0, experts, experts, sums_tall)
    fill(2, 0, experts)
    sums_side(1)
    for g in high[:1]:
        next_group(g, experts)
    sums_across(1)
    for g in high[1:]:
        next_group(g, experts)
    fill(1, 0, experts)
    sums_back(1)
    send_across(inner, [(0, g, k) for g in low for k in range(1, half_chips)])
    own(0, 0, experts)
    router_copy(facing, facing).wait_recv()
    for k in range(1, half):
        forward_copy(side * half + mate(k), me).start()
    sums_done(1)
    send_across(inner, [(0, g, k) for g in high for k in range(1, half_chips)])
    for t, body in ((1, ready_wide(1)), (2, ready_tall)):
        for g in range(len(groups[t])):
            ready(t, g, experts, body)
            send_across(inner, [(t, g, k) for k in range(half_chips) if (t, g, k) != (*last, 0)])
            send_side(t, g)

    start, size = groups[2][-1]
    for c in range(CORES):
        late_send[c] = send_tall[across * CORES + c, pl.ds(start, size)]
    for t in (1, 2):
        own(t, 0, experts)

    for k in range(1, half):
        other = side * half + mate(k)
        router_copy(other, other).wait_recv()
        forward_copy(other, other).wait_recv()
    for k in range(1, owners):
        col_copy(lax.rem(home + k, owners), home).start()

    before = (2, last[1] - 1)

    @pl.when(outer)
    def _():
        for c in range(CORES):
            block_copy(*before, across * CORES + c, across * CORES + c).wait_recv()
        for g in held:
            send_side(0, g)

    for k in range(half_chips):
        send_across(outer, [(t, g, k) for t in range(3) for g in range(len(groups[t]))])

    for k in range(1, owners):
        other = lax.rem(home + k, owners)
        col_copy(other, other).wait_recv()
        col_copy(other, home).wait_send()
    router_copy(facing, me).wait_send()
    for k in range(1, half):
        other = side * half + mate(k)
        router_copy(other, me).wait_send()
        forward_copy(other, me).wait_send()
        for s in range(2):
            side_copy(s, mate(k), member).wait_send()
            total_copy(s, mate(k), member).wait_send()
    for s in range(2):
        half_copy(s).wait_send()
    for to in reach:

        @pl.when(me != to)
        def _():
            early_copy(to, me).wait_send()

    for t in range(3):
        for g in range(len(groups[t])):

            @pl.loop(1, n)
            def _(k):
                other = peer(k)
                facing_chip = other // CORES == across
                if (t, g) == before:

                    @pl.when(jnp.logical_not(facing_chip & outer))
                    def _():
                        block_copy(t, g, other, other).wait_recv()

                    block_copy(t, g, other, me).wait_send()
                elif (t, g) == last:

                    @pl.when(jnp.logical_not(facing_chip & inner))
                    def _():
                        block_copy(t, g, other, other).wait_recv()
                        block_copy(t, g, other, me).wait_send()
                else:
                    block_copy(t, g, other, other).wait_recv()
                    block_copy(t, g, other, me).wait_send()


def late_exchange(n, late_send, _, late_got, send_sem, recv_sem):
    me = lax.axis_index("rows")
    _, inner, across = sides(n, me)
    core = lax.rem(me, CORES)

    def copy(to, src):
        return pltpu.make_async_remote_copy(
            src_ref=late_send.at[to],
            dst_ref=late_got.at[src],
            send_sem=send_sem.at[to],
            recv_sem=recv_sem.at[src],
            device_id={"rows": across * CORES + to},
            device_id_type=MESH,
        )

    @pl.when(inner)
    def _():
        barrier = pltpu.get_barrier_semaphore()
        for c in range(CORES):
            pl.semaphore_signal(
                barrier, inc=1, device_id={"rows": across * CORES + c}, device_id_type=MESH
            )
        pl.semaphore_wait(barrier, CORES)
        for c in range(CORES):
            copy(lax.rem(core + c, CORES), core).start()
        for c in range(CORES):
            copy(c, c).wait_recv()
            copy(c, core).wait_send()


def late_place(n, start, late_got, down, out, sem):
    me = lax.axis_index("rows")
    _, inner, across = sides(n, me)
    size, rows = late_got.shape[1], late_got.shape[3]

    @pl.when(inner)
    def _():
        copies = []
        for c in range(CORES):
            src = across * CORES + c
            at = pl.ds(pl.multiple_of(src * rows, rows), rows)
            copies.append(
                pltpu.make_async_copy(
                    late_got.at[c], out.at[pl.ds(start, size), :, at], sem.at[c]
                )
            )
        for copy in copies:
            copy.start()
        for copy in copies:
            copy.wait()


def chunks_of(shape):
    count = CHUNKS if len(shape) == 3 and shape[0] % CHUNKS == 0 else 1
    size = shape[0] // count
    return [pl.ds(i * size, size) for i in range(count)]


def write_back(count, *refs):
    ins, outs, sem = refs[:count], refs[count : 2 * count], refs[2 * count]
    copies = []
    for i, (a, b) in enumerate(zip(ins, outs)):
        for j, some in enumerate(chunks_of(a.shape)):
            copies.append(pltpu.make_async_copy(a.at[some], b.at[some], sem.at[i, j]))
    for copy in copies:
        copy.start()
    for copy in copies:
        copy.wait()


def local(n, owners, gate, up, down, router_weight, router_gain):
    experts, rows, width = gate.shape
    share = width // n
    half = n // 2
    pair = 2 * share
    early, groups, _, total_groups = plan(experts)
    slots = min(SLOTS, experts)
    router = router_weight.T
    gain = router_gain.reshape(1, -1)
    columns = router.shape[0]
    anywhere = pl.BlockSpec(memory_space=pl.ANY)
    vmem = pl.BlockSpec(memory_space=pltpu.VMEM)
    hbm = pl.BlockSpec(memory_space=pltpu.HBM)
    f32, bf16 = jnp.float32, jnp.bfloat16
    dma = pltpu.SemaphoreType.DMA
    shapes = (
        ((experts, rows * n, share), bf16),
        ((experts, rows * n, share), bf16),
        ((experts, share, rows * n), bf16),
        ((experts, share), f32),
        ((experts, share), f32),
        ((experts, share), f32),
        ((owners, columns, rows * n), bf16),
    )
    start, size = groups[2][-1]
    late = ((CORES, size, share, rows), bf16)
    *results, late_send = pl.pallas_call(
        functools.partial(exchange, n, owners),
        name="exchange",
        out_shape=tuple(pltpu.VMEM(*s) for s in (*shapes, late)),
        in_specs=[anywhere] * 5,
        out_specs=(vmem,) * (len(shapes) + 1),
        scratch_shapes=[
            pltpu.VMEM((early, rows, width), f32),
            pltpu.VMEM((slots, rows, width), f32),
            pltpu.VMEM((slots, width, rows), f32),
            pltpu.VMEM((2, n, experts, rows, share), bf16),
            pltpu.VMEM((n, experts, share, rows), bf16),
            pltpu.VMEM((2, early, width // 2), f32),
            pltpu.VMEM((n, early, width // 2), f32),
            pltpu.VMEM((early, width // 2), f32),
            pltpu.VMEM((half, 3, experts, pair), f32),
            pltpu.VMEM((half, 3, experts, pair), f32),
            pltpu.VMEM((3, experts, pair), f32),
            pltpu.VMEM((3, experts, pair), f32),
            pltpu.VMEM((half, 3, experts, pair), f32),
            pltpu.VMEM((half, 3, experts, pair), f32),
            pltpu.VMEM((columns, rows), f32),
            pltpu.VMEM((1, rows), f32),
            pltpu.VMEM((columns, rows), bf16),
            dma((4, max(slots, 2, early))),
            dma((n,)),
            dma((n,)),
            dma((2, half)),
            dma((2, half)),
            dma((2,)),
            dma((2,)),
            dma((2, half)),
            dma((2, half)),
            dma((n,)),
            dma((n,)),
            dma((n,)),
            dma((n,)),
            dma((owners,)),
            dma((owners,)),
            dma((total_groups, n)),
            dma((total_groups, n)),
        ],
        compiler_params=pltpu.CompilerParams(
            collective_id=0, has_side_effects=True, vmem_limit_bytes=38 * 1024 * 1024
        ),
    )(gate, up, down, router, gain)
    outs = pl.pallas_call(
        functools.partial(write_back, len(shapes)),
        name="write_back",
        out_shape=tuple(pltpu.HBM(*s) for s in shapes),
        in_specs=[vmem] * len(shapes),
        out_specs=(hbm,) * len(shapes),
        scratch_shapes=[dma((len(shapes), CHUNKS))],
        compiler_params=pltpu.CompilerParams(vmem_limit_bytes=1024 * 1024),
    )(*results)
    late_got = pl.pallas_call(
        functools.partial(late_exchange, n),
        name="late_exchange",
        out_shape=pltpu.VMEM(*late),
        in_specs=[vmem, anywhere],
        out_specs=vmem,
        scratch_shapes=[dma((CORES,)), dma((CORES,))],
        compiler_params=pltpu.CompilerParams(
            collective_id=1, has_side_effects=True, vmem_limit_bytes=1024 * 1024
        ),
    )(late_send, outs[3])
    ready_down = pl.pallas_call(
        functools.partial(late_place, n, start),
        name="late_place",
        out_shape=pltpu.HBM(*shapes[2]),
        in_specs=[vmem, hbm],
        out_specs=hbm,
        scratch_shapes=[dma((CORES,))],
        input_output_aliases={1: 0},
        compiler_params=pltpu.CompilerParams(vmem_limit_bytes=1024 * 1024),
    )(late_got, outs[2])
    serve_router = outs[6].reshape(owners * columns, rows * n).T
    return (*outs[:2], ready_down, *outs[3:6], serve_router)


def solution(mesh):
    return jax.shard_map(
        functools.partial(local, mesh.shape["rows"], mesh.shape["owner"]),
        mesh=mesh,
        in_specs=(
            P("owner", "rows", None),
            P("owner", "rows", None),
            P("owner", None, "rows"),
            P("rows", "owner"),
            P("rows"),
        ),
        out_specs=(
            P("owner", None, "rows"),
            P("owner", None, "rows"),
            P("owner", "rows", None),
            P("owner", "rows"),
            P("owner", "rows"),
            P("owner", "rows"),
            P(),
        ),
        check_vma=False,
    )
```

```python
import functools

import jax
import jax.numpy as jnp
from jax import lax
from jax.experimental import pallas as pl
from jax.experimental.pallas import tpu as pltpu
from jax.sharding import PartitionSpec as P

CORES = 2
SLOTS = 4
EARLY = 3
SHADOW = 6
CHUNKS = 4
GROUPS = 4
MESH = pl.DeviceIdType.MESH


def groups_of(experts, start):
    per = max(1, experts // GROUPS)
    out = [(e, 1) for e in range(start)]
    at = start
    while at < experts:
        end = min(experts, (at // per + 1) * per)
        out.append((at, end - at))
        at = end
    return out


def plan(experts):
    early = max(1, min(EARLY, experts // 4))
    groups = [groups_of(experts, early), groups_of(experts, 0), groups_of(experts, 0)]
    (start, size), (_, more) = groups[2][-2:]
    groups[2][-2:] = [(start, size + more)]
    base = [0, len(groups[0]), len(groups[0]) + len(groups[1])]
    return early, groups, base, sum(len(g) for g in groups)


def sides(n, me):
    chips = n // CORES
    chip = me // CORES
    inner = (chip == chips // 2 - 1) | (chip == chips // 2)
    return chip, inner, jnp.where(chip < chips // 2, chips // 2, chips // 2 - 1)


def exchange(
    n,
    owners,
    gate,
    up,
    down,
    router_weight,
    router_gain,
    out_gate,
    out_up,
    out_down,
    scale_gate,
    scale_up,
    scale_down,
    out_router,
    late_send,
    first,
    wide,
    tall,
    send_wide,
    send_tall,
    early_part,
    early_got,
    early_inv,
    raw_got,
    part,
    got_side,
    half_sum,
    got_half,
    total,
    inverse,
    weight,
    gain,
    router,
    load_sem,
    early_send,
    early_recv,
    raw_sem,
    side_send,
    side_recv,
    half_send,
    half_recv,
    total_send,
    total_recv,
    router_send,
    router_recv,
    fwd_send,
    fwd_recv,
    col_send,
    col_recv,
    bulk_send,
    bulk_recv,
    through,
):
    me = lax.axis_index("rows")
    home = lax.axis_index("owner")
    experts, rows, width = gate.shape
    share = width // n
    pair = 2 * share
    half = n // 2
    slots = wide.shape[0]
    chips = n // CORES
    half_chips = chips // 2
    chip, inner, across = sides(n, me)
    core = lax.rem(me, CORES)
    side = me // half
    member = lax.rem(me, half)
    facing = lax.rem(me + half, n)
    early, groups, base, _ = plan(experts)
    count = rows * n
    srcs = (gate, up, down)
    span = pl.ds(pl.multiple_of(me * rows, rows), rows)

    def peer(k):
        return lax.rem(me + k, n)

    def mate(k):
        return lax.rem(member + k, half)

    def remote(src, dst, out_sem, in_sem, **where):
        return pltpu.make_async_remote_copy(
            src_ref=src,
            dst_ref=dst,
            send_sem=out_sem,
            recv_sem=in_sem,
            device_id=where,
            device_id_type=MESH,
        )

    def load(t, e):
        buf = wide if t < 2 else tall
        slot = lax.rem(e, slots)
        return pltpu.make_async_copy(
            srcs[t].at[e], buf.at[slot], load_sem.at[0 if t < 2 else 1, slot]
        )

    def load_first(e):
        return pltpu.make_async_copy(gate.at[e], first.at[e], load_sem.at[2, e])

    for e in range(early):
        load_first(e).start()

    def fill(t, start, stop):
        for e in range(start, min(start + slots, stop)):
            load(t, e).start()

    def run(t, start, stop, last, body):
        @pl.loop(start, stop)
        def _(e):
            load(t, e).wait()
            body(e, lax.rem(e, slots))

            @pl.when(e + slots < last)
            def _():
                load(t, e + slots).start()

    fill(0, early, experts)
    weight_load = pltpu.make_async_copy(router_weight, weight, load_sem.at[3, 0])
    gain_load = pltpu.make_async_copy(router_gain, gain, load_sem.at[3, 1])
    weight_load.start()
    gain_load.start()

    barrier = pltpu.get_barrier_semaphore()
    for k in range(1, n):
        pl.semaphore_signal(barrier, inc=1, device_id={"rows": peer(k)}, device_id_type=MESH)
    for k in range(1, owners):
        pl.semaphore_signal(
            barrier, inc=1, device_id={"owner": lax.rem(home + k, owners)}, device_id_type=MESH
        )

    def put_part(t, e, sums):
        for q in range(half):
            part[q, t, pl.ds(e, 1), :] = sums[:, q * pair : (q + 1) * pair]

    def sums_wide(t):
        def body(e, slot):
            put_part(t, e, jnp.sum(jnp.abs(wide[slot]), axis=0, keepdims=True))

        return body

    def sums_tall(e, slot):
        for q in range(half):
            block = jnp.abs(tall[slot, q * pair : (q + 1) * pair, :])
            folded = block[:, :128]
            for c in range(128, rows, 128):
                folded = folded + block[:, c : c + 128]
            part[q, 2, pl.ds(e, 1), :] = jnp.sum(folded.T, axis=0, keepdims=True)

    for e in range(early):
        load_first(e).wait()
        sums = jnp.sum(jnp.abs(first[e]), axis=0, keepdims=True)
        put_part(0, e, sums)
        for s in range(2):
            early_part[s, e] = sums[:, s * (width // 2) : (s + 1) * (width // 2)]

    pl.semaphore_wait(barrier, n - 1 + owners - 1)

    inners = (half_chips - 1, half_chips)
    reach = [c * CORES + i for c in inners for i in range(CORES)]

    early_some = [pl.ds(0, 1)] + [pl.ds(1, early - 1)] * (early > 1)

    def early_copy(i, to, src):
        return remote(
            early_part.at[1 - to // half, early_some[i]],
            early_got.at[src, early_some[i]],
            early_send.at[i, to],
            early_recv.at[i, src],
            rows=to,
        )

    def early_sums(i):
        for to in reach:

            @pl.when(me != to)
            def _():
                early_copy(i, to, me).start()

    early_sums(0)

    raw = share % 128 == 0
    partner = across * CORES + core

    def raw_copy():
        return remote(
            first.at[0, :, pl.ds(pl.multiple_of(partner * share, share), share)],
            raw_got,
            raw_sem.at[0],
            raw_sem.at[1],
            rows=partner,
        )

    if raw:

        @pl.when(inner)
        def _():
            raw_copy().start()

    for i in range(1, len(early_some)):
        early_sums(i)

    weight_load.wait()
    gain_load.wait()
    router[...] = (weight[...] * gain[...]).astype(jnp.bfloat16)
    out_router[home, :, span] = router[...]

    def strip(src):
        return out_router.at[home, :, pl.ds(pl.multiple_of(src * rows, rows), rows)]

    def router_copy(to, src):
        return remote(router, strip(src), router_send.at[to], router_recv.at[src], rows=to)

    def forward_copy(to, src):
        return remote(
            strip(lax.rem(src + half, n)),
            strip(lax.rem(src + half, n)),
            fwd_send.at[to],
            fwd_recv.at[src],
            rows=to,
        )

    def col_copy(to, src):
        return remote(
            out_router.at[src], out_router.at[src], col_send.at[to], col_recv.at[src], owner=to
        )

    for k in range(1, half):
        router_copy(side * half + mate(k), me).start()
    router_copy(facing, me).start()

    shadow = min(early + SHADOW, experts)
    run(0, early, shadow, experts, sums_wide(0))

    stages = (pl.ds(0, 1), pl.ds(1, 2))

    def side_copy(s, to, src):
        return remote(
            part.at[to, stages[s]],
            got_side.at[src, stages[s]],
            side_send.at[s, to],
            side_recv.at[s, src],
            rows=side * half + to,
        )

    def half_copy(s):
        return remote(
            half_sum.at[stages[s]],
            got_half.at[stages[s]],
            half_send.at[s],
            half_recv.at[s],
            rows=facing,
        )

    def total_copy(s, to, src):
        block = total.at[src, stages[s]]
        return remote(
            block, block, total_send.at[s, to], total_recv.at[s, src], rows=side * half + to
        )

    def sums_side(s):
        for k in range(1, half):
            side_copy(s, mate(k), member).start()

    def sums_across(s):
        acc = part[member, stages[s]]
        for k in range(1, half):
            side_copy(s, mate(k), mate(k)).wait_recv()
            acc = acc + got_side[mate(k), stages[s]]
        half_sum[stages[s]] = acc
        half_copy(s).start()

    def sums_back(s):
        half_copy(s).wait_recv()
        total[member, stages[s]] = half_sum[stages[s]] + got_half[stages[s]]
        for k in range(1, half):
            total_copy(s, mate(k), member).start()

    scales = (scale_gate, scale_up, scale_down)

    def sums_done(s):
        for k in range(1, half):
            total_copy(s, mate(k), mate(k)).wait_recv()
        for t in ((0,), (1, 2))[s]:
            for q in range(half):
                inverse[q, t] = 1.0 / (total[q, t] / count)
            mine = total[me // 2, t] / count
            scales[t][...] = jnp.where(lax.rem(me, 2) == 0, mine[:, :share], mine[:, share:])

    def block_copy(t, g, to, src):
        start, size = groups[t][g]
        some = pl.ds(start, size)
        at = pl.ds(pl.multiple_of(src * rows, rows), rows)
        if t < 2:
            piece = send_wide.at[t, to, some]
            dst = (out_gate, out_up)[t].at[some, at, :]
        else:
            piece = send_tall.at[to, some]
            dst = out_down.at[some, :, at]
        b = base[t] + g
        return remote(piece, dst, bulk_send.at[b, to], bulk_recv.at[b, src], rows=to)

    def send_chip(t, g, there, cores=range(CORES)):
        for c in cores:
            block_copy(t, g, there * CORES + lax.rem(core + c, CORES), me).start()

    def send_side(t, g):
        for d in range(1, half_chips):
            for way in (1, -1):
                there = chip + way * d

                @pl.when((there // half_chips == chip // half_chips) & (there >= 0))
                def _():
                    send_chip(t, g, there)

        for c in range(1, CORES):
            block_copy(t, g, chip * CORES + lax.rem(core + c, CORES), me).start()

    last = (2, len(groups[2]) - 1)

    tail = (0, early - 1, half_chips - 1)
    tail_chip = jnp.where(side == 0, chips - 1, 0)
    tail_to = tail_chip * CORES + lax.rem(core + CORES - 1, CORES)

    def send_across(who, pieces):
        @pl.when(who)
        def _():
            for t, g, k in pieces:
                there = jnp.where(side == 0, half_chips + k, half_chips - 1 - k)
                if who is inner and (t, g, k) == tail:
                    send_chip(t, g, there, range(CORES - 1))
                else:
                    send_chip(t, g, there)

    def scaled_pair(t, e, q, block, factor):
        value = (block * factor).astype(jnp.bfloat16)
        for i in range(2):
            send_wide[t, 2 * q + i, e] = value[:, i * share : (i + 1) * share]

    def half_first(e, which, factor_of):
        for p in range(half // 2):
            q = which * (half // 2) + p
            at = pl.ds(pl.multiple_of(q * pair, pair), pair)
            scaled_pair(0, e, q, first[e, :, at], factor_of(p, q))

    def early_factor(e):
        return lambda p, q: early_inv[e, :, p * pair : (p + 1) * pair]

    def late_factor(e):
        return lambda p, q: inverse[q, 0, pl.ds(e, 1), :]

    def ready_wide(t):
        def body(e, slot):
            for q in range(half):
                scaled_pair(
                    t,
                    e,
                    q,
                    wide[slot, :, q * pair : (q + 1) * pair],
                    inverse[q, t, pl.ds(e, 1), :],
                )

        return body

    def ready_tall(e, slot):
        for q in range(half):
            row = inverse[q, 2, pl.ds(e, 1), :]
            factor = jnp.broadcast_to(row, (128, pair)).T
            for c in range(0, rows, 128):
                block = tall[slot, q * pair : (q + 1) * pair, c : c + 128]
                value = (block * factor).astype(jnp.bfloat16)
                for i in range(2):
                    send_tall[2 * q + i, e, :, c : c + 128] = value[
                        i * share : (i + 1) * share
                    ]

    def own(t, start, stop):
        @pl.loop(start, stop)
        def _(e):
            if t < 2:
                (out_gate, out_up)[t][e, span, :] = send_wide[t, me, e]
            else:
                out_down[e, :, span] = send_tall[me, e]

    def ready(t, g, last, body):
        start, size = groups[t][g]
        run(t, start, start + size, last, body)

    def early_inverse(i):
        @pl.when(inner)
        def _():
            acc = early_part[1 - side, early_some[i]]
            for k in range(1, n):
                early_copy(i, peer(k), peer(k)).wait_recv()
                acc = acc + early_got[peer(k), early_some[i]]
            early_inv[early_some[i]] = 1.0 / (acc / count)

    early_inverse(0)
    pieces = [(0, e, k) for k in range(half_chips) for e in range(early)]
    outer = jnp.logical_not(inner)
    middle = experts // 2
    rest = range(early, len(groups[0]))
    low = [g for g in rest if groups[0][g][0] < middle]
    high = [g for g in rest if groups[0][g][0] >= middle]

    def early_ready(e):
        @pl.when(inner)
        def _():
            half_first(e, 1 - side, early_factor(e))

    early_ready(0)
    if raw:

        @pl.when(inner)
        def _():
            send_chip(0, 0, across, range(1, CORES))

    send_across(inner, pieces[raw:1])
    run(0, shadow, experts, experts, sums_wide(0))
    fill(1, 0, middle)
    sums_side(0)
    for i in range(1, len(early_some)):
        early_inverse(i)
    for e in range(1, early):
        early_ready(e)
    send_across(inner, pieces[1:2])
    sums_across(0)
    send_across(inner, pieces[2:4])
    run(1, 0, middle, middle, sums_wide(1))
    fill(0, early, middle)
    fill(2, 0, experts)
    sums_back(0)
    send_across(inner, pieces[4:])
    sums_done(0)

    def next_group(g, stop):
        ready(0, g, stop, ready_wide(0))
        send_across(inner, [(0, g, 0)])
        send_side(0, g)

    for g in low:
        next_group(g, middle)
    fill(1, middle, experts)
    for e in range(early):
        half_first(e, side, late_factor(e))

        @pl.when(outer)
        def _():
            half_first(e, 1 - side, late_factor(e))

    for g in range(early):
        send_side(0, g)
    run(1, middle, experts, experts, sums_wide(1))
    fill(0, middle, experts)
    run(2, 0, experts, experts, sums_tall)
    fill(2, 0, experts)
    sums_side(1)
    for g in high[:1]:
        next_group(g, experts)
    sums_across(1)
    for g in high[1:]:
        next_group(g, experts)
    fill(1, 0, experts)
    sums_back(1)
    send_across(inner, [(0, g, k) for g in low for k in range(1, half_chips)])
    own(0, 0, experts)
    router_copy(facing, facing).wait_recv()
    for k in range(1, half):
        forward_copy(side * half + mate(k), me).start()
    sums_done(1)
    send_across(inner, [(0, g, k) for g in high for k in range(1, half_chips)])
    for t, body in ((1, ready_wide(1)), (2, ready_tall)):
        for g in range(len(groups[t])):
            ready(t, g, experts, body)
            send_across(inner, [(t, g, k) for k in range(half_chips) if (t, g, k) != (*last, 0)])
            send_side(t, g)

    start, size = groups[2][-1]
    for c in range(CORES):
        late_send[c] = send_tall[across * CORES + c, pl.ds(start, size)]
    for t in (1, 2):
        own(t, 0, experts)

    if raw:

        @pl.when(inner)
        def _():
            raw_copy().wait_recv()
            row = inverse[me // 2, 0, pl.ds(0, 1), :]
            mine = jnp.where(lax.rem(me, 2) == 0, row[:, :share], row[:, share:])
            at = pl.ds(pl.multiple_of(partner * rows, rows), rows)
            out_gate[0, at, :] = (raw_got[...] * mine).astype(jnp.bfloat16)
            raw_copy().wait_send()

    for k in range(1, half):
        other = side * half + mate(k)
        router_copy(other, other).wait_recv()
        forward_copy(other, other).wait_recv()
    for k in range(1, owners):
        col_copy(lax.rem(home + k, owners), home).start()

    @pl.when(inner)
    def _():
        send_chip(*tail[:2], tail_chip, range(CORES - 1, CORES))

    def kept(t, g, other):
        facing_chip = (other // CORES == across) & inner
        if (t, g) == last:
            return facing_chip
        if raw and (t, g) == (0, 0):
            return facing_chip & (other == partner)
        return None

    def unless(skip, body):
        if skip is None:
            body()
        else:
            pl.when(jnp.logical_not(skip))(body)

    outers = [c for c in range(half_chips - 1)]

    @pl.when(inner)
    def _():
        for t in range(3):
            for g in range(len(groups[t])):

                @pl.loop(0, half)
                def _(m):
                    other = (1 - side) * half + m
                    skip = kept(t, g, other)
                    if (t, g) == tail[:2]:
                        skip = (other == tail_to) if skip is None else skip | (other == tail_to)
                    unless(skip, lambda: block_copy(t, g, other, me).wait_send())

        for i in outers:
            there = jnp.where(side == 0, i, chips - 1 - i)
            for c in range(CORES):
                pl.semaphore_signal(
                    through, inc=1, device_id={"rows": there * CORES + c}, device_id_type=MESH
                )

        block_copy(*tail[:2], tail_to, me).wait_send()

    @pl.when(outer)
    def _():
        pl.semaphore_wait(through, CORES)

    for k in range(half_chips):
        send_across(outer, [(t, g, k) for t in range(3) for g in range(len(groups[t]))])

    for k in range(1, owners):
        other = lax.rem(home + k, owners)
        col_copy(other, other).wait_recv()
        col_copy(other, home).wait_send()
    router_copy(facing, me).wait_send()
    for k in range(1, half):
        other = side * half + mate(k)
        router_copy(other, me).wait_send()
        forward_copy(other, me).wait_send()
        for s in range(2):
            side_copy(s, mate(k), member).wait_send()
            total_copy(s, mate(k), member).wait_send()
    for s in range(2):
        half_copy(s).wait_send()
    for i in range(len(early_some)):
        for to in reach:

            @pl.when(me != to)
            def _():
                early_copy(i, to, me).wait_send()

    for t in range(3):
        for g in range(len(groups[t])):

            @pl.loop(1, n)
            def _(k):
                other = peer(k)
                unless(kept(t, g, other), lambda: block_copy(t, g, other, other).wait_recv())

                @pl.when(jnp.logical_not(inner & (other // half != side)))
                def _():
                    block_copy(t, g, other, me).wait_send()


def late_exchange(n, late_send, _, late_got, send_sem, recv_sem):
    me = lax.axis_index("rows")
    _, inner, across = sides(n, me)
    core = lax.rem(me, CORES)

    def copy(to, src):
        return pltpu.make_async_remote_copy(
            src_ref=late_send.at[to],
            dst_ref=late_got.at[src],
            send_sem=send_sem.at[to],
            recv_sem=recv_sem.at[src],
            device_id={"rows": across * CORES + to},
            device_id_type=MESH,
        )

    @pl.when(inner)
    def _():
        barrier = pltpu.get_barrier_semaphore()
        for c in range(CORES):
            pl.semaphore_signal(
                barrier, inc=1, device_id={"rows": across * CORES + c}, device_id_type=MESH
            )
        pl.semaphore_wait(barrier, CORES)
        for c in range(CORES):
            copy(lax.rem(core + c, CORES), core).start()
        for c in range(CORES):
            copy(c, c).wait_recv()
            copy(c, core).wait_send()


def late_place(n, start, late_got, down, out, sem):
    me = lax.axis_index("rows")
    _, inner, across = sides(n, me)
    size, rows = late_got.shape[1], late_got.shape[3]

    @pl.when(inner)
    def _():
        copies = []
        for c in range(CORES):
            src = across * CORES + c
            at = pl.ds(pl.multiple_of(src * rows, rows), rows)
            copies.append(
                pltpu.make_async_copy(
                    late_got.at[c], out.at[pl.ds(start, size), :, at], sem.at[c]
                )
            )
        for copy in copies:
            copy.start()
        for copy in copies:
            copy.wait()


def chunks_of(shape):
    count = CHUNKS if len(shape) == 3 and shape[0] % CHUNKS == 0 else 1
    size = shape[0] // count
    return [pl.ds(i * size, size) for i in range(count)]


def write_back(count, *refs):
    ins, outs, sem = refs[:count], refs[count : 2 * count], refs[2 * count]
    copies = []
    for i, (a, b) in enumerate(zip(ins, outs)):
        for j, some in enumerate(chunks_of(a.shape)):
            copies.append(pltpu.make_async_copy(a.at[some], b.at[some], sem.at[i, j]))
    for copy in copies:
        copy.start()
    for copy in copies:
        copy.wait()


def local(n, owners, gate, up, down, router_weight, router_gain):
    experts, rows, width = gate.shape
    share = width // n
    half = n // 2
    pair = 2 * share
    early, groups, _, total_groups = plan(experts)
    slots = min(SLOTS, experts)
    router = router_weight.T
    gain = router_gain.reshape(1, -1)
    columns = router.shape[0]
    anywhere = pl.BlockSpec(memory_space=pl.ANY)
    vmem = pl.BlockSpec(memory_space=pltpu.VMEM)
    hbm = pl.BlockSpec(memory_space=pltpu.HBM)
    f32, bf16 = jnp.float32, jnp.bfloat16
    dma = pltpu.SemaphoreType.DMA
    shapes = (
        ((experts, rows * n, share), bf16),
        ((experts, rows * n, share), bf16),
        ((experts, share, rows * n), bf16),
        ((experts, share), f32),
        ((experts, share), f32),
        ((experts, share), f32),
        ((owners, columns, rows * n), bf16),
    )
    start, size = groups[2][-1]
    late = ((CORES, size, share, rows), bf16)
    *results, late_send = pl.pallas_call(
        functools.partial(exchange, n, owners),
        name="exchange",
        out_shape=tuple(pltpu.VMEM(*s) for s in (*shapes, late)),
        in_specs=[anywhere] * 5,
        out_specs=(vmem,) * (len(shapes) + 1),
        scratch_shapes=[
            pltpu.VMEM((early, rows, width), f32),
            pltpu.VMEM((slots, rows, width), f32),
            pltpu.VMEM((slots, width, rows), f32),
            pltpu.VMEM((2, n, experts, rows, share), bf16),
            pltpu.VMEM((n, experts, share, rows), bf16),
            pltpu.VMEM((2, early, 1, width // 2), f32),
            pltpu.VMEM((n, early, 1, width // 2), f32),
            pltpu.VMEM((early, 1, width // 2), f32),
            pltpu.VMEM((rows, share), f32),
            pltpu.VMEM((half, 3, experts, pair), f32),
            pltpu.VMEM((half, 3, experts, pair), f32),
            pltpu.VMEM((3, experts, pair), f32),
            pltpu.VMEM((3, experts, pair), f32),
            pltpu.VMEM((half, 3, experts, pair), f32),
            pltpu.VMEM((half, 3, experts, pair), f32),
            pltpu.VMEM((columns, rows), f32),
            pltpu.VMEM((1, rows), f32),
            pltpu.VMEM((columns, rows), bf16),
            dma((4, max(slots, 2, early))),
            dma((2, n)),
            dma((2, n)),
            dma((2,)),
            dma((2, half)),
            dma((2, half)),
            dma((2,)),
            dma((2,)),
            dma((2, half)),
            dma((2, half)),
            dma((n,)),
            dma((n,)),
            dma((n,)),
            dma((n,)),
            dma((owners,)),
            dma((owners,)),
            dma((total_groups, n)),
            dma((total_groups, n)),
            pltpu.SemaphoreType.REGULAR,
        ],
        compiler_params=pltpu.CompilerParams(
            collective_id=0, has_side_effects=True, vmem_limit_bytes=38 * 1024 * 1024
        ),
    )(gate, up, down, router, gain)
    outs = pl.pallas_call(
        functools.partial(write_back, len(shapes)),
        name="write_back",
        out_shape=tuple(pltpu.HBM(*s) for s in shapes),
        in_specs=[vmem] * len(shapes),
        out_specs=(hbm,) * len(shapes),
        scratch_shapes=[dma((len(shapes), CHUNKS))],
        compiler_params=pltpu.CompilerParams(vmem_limit_bytes=1024 * 1024),
    )(*results)
    late_got = pl.pallas_call(
        functools.partial(late_exchange, n),
        name="late_exchange",
        out_shape=pltpu.VMEM(*late),
        in_specs=[vmem, anywhere],
        out_specs=vmem,
        scratch_shapes=[dma((CORES,)), dma((CORES,))],
        compiler_params=pltpu.CompilerParams(
            collective_id=1, has_side_effects=True, vmem_limit_bytes=1024 * 1024
        ),
    )(late_send, outs[3])
    ready_down = pl.pallas_call(
        functools.partial(late_place, n, start),
        name="late_place",
        out_shape=pltpu.HBM(*shapes[2]),
        in_specs=[vmem, hbm],
        out_specs=hbm,
        scratch_shapes=[dma((CORES,))],
        input_output_aliases={1: 0},
        compiler_params=pltpu.CompilerParams(vmem_limit_bytes=1024 * 1024),
    )(late_got, outs[2])
    serve_router = outs[6].reshape(owners * columns, rows * n).T
    return (*outs[:2], ready_down, *outs[3:6], serve_router)


def solution(mesh):
    return jax.shard_map(
        functools.partial(local, mesh.shape["rows"], mesh.shape["owner"]),
        mesh=mesh,
        in_specs=(
            P("owner", "rows", None),
            P("owner", "rows", None),
            P("owner", None, "rows"),
            P("rows", "owner"),
            P("rows"),
        ),
        out_specs=(
            P("owner", None, "rows"),
            P("owner", None, "rows"),
            P("owner", "rows", None),
            P("owner", "rows"),
            P("owner", "rows"),
            P("owner", "rows"),
            P(),
        ),
        check_vma=False,
    )
```

```python
import functools

import jax
import jax.numpy as jnp
from jax import lax
from jax.experimental import pallas as pl
from jax.experimental.pallas import tpu as pltpu
from jax.sharding import PartitionSpec as P

CORES = 2
SLOTS = 4
EARLY = 3
SHADOW = 10
CHUNKS = 4
GROUPS = 4
MESH = pl.DeviceIdType.MESH


def groups_of(experts, start):
    per = max(1, experts // GROUPS)
    out = [(e, 1) for e in range(start)]
    at = start
    while at < experts:
        end = min(experts, (at // per + 1) * per)
        out.append((at, end - at))
        at = end
    return out


def plan(experts):
    early = max(1, min(EARLY, experts // 4))
    groups = [groups_of(experts, early), groups_of(experts, 0), groups_of(experts, 0)]
    (start, size), (_, more) = groups[2][-2:]
    groups[2][-2:] = [(start, size + more)]
    base = [0, len(groups[0]), len(groups[0]) + len(groups[1])]
    return early, groups, base, sum(len(g) for g in groups)


def sides(n, me):
    chips = n // CORES
    chip = me // CORES
    inner = (chip == chips // 2 - 1) | (chip == chips // 2)
    return chip, inner, jnp.where(chip < chips // 2, chips // 2, chips // 2 - 1)


def exchange(
    n,
    owners,
    gate,
    up,
    down,
    router_weight,
    router_gain,
    out_gate,
    out_up,
    out_down,
    scale_gate,
    scale_up,
    scale_down,
    out_router,
    late_send,
    first,
    wide,
    tall,
    send_wide,
    send_tall,
    early_part,
    early_got,
    early_inv,
    raw_got,
    part,
    got_side,
    half_sum,
    got_half,
    total,
    inverse,
    weight,
    gain,
    router,
    load_sem,
    early_send,
    early_recv,
    raw_sem,
    side_send,
    side_recv,
    half_send,
    half_recv,
    total_send,
    total_recv,
    router_send,
    router_recv,
    fwd_send,
    fwd_recv,
    col_send,
    col_recv,
    bulk_send,
    bulk_recv,
    through,
):
    me = lax.axis_index("rows")
    home = lax.axis_index("owner")
    experts, rows, width = gate.shape
    share = width // n
    pair = 2 * share
    half = n // 2
    slots = wide.shape[0]
    chips = n // CORES
    half_chips = chips // 2
    chip, inner, across = sides(n, me)
    core = lax.rem(me, CORES)
    side = me // half
    member = lax.rem(me, half)
    facing = lax.rem(me + half, n)
    early, groups, base, _ = plan(experts)
    count = rows * n
    srcs = (gate, up, down)
    span = pl.ds(pl.multiple_of(me * rows, rows), rows)

    def peer(k):
        return lax.rem(me + k, n)

    def mate(k):
        return lax.rem(member + k, half)

    def remote(src, dst, out_sem, in_sem, **where):
        return pltpu.make_async_remote_copy(
            src_ref=src,
            dst_ref=dst,
            send_sem=out_sem,
            recv_sem=in_sem,
            device_id=where,
            device_id_type=MESH,
        )

    def load(t, e):
        buf = wide if t < 2 else tall
        slot = lax.rem(e, slots)
        return pltpu.make_async_copy(
            srcs[t].at[e], buf.at[slot], load_sem.at[0 if t < 2 else 1, slot]
        )

    def load_first(e):
        return pltpu.make_async_copy(gate.at[e], first.at[e], load_sem.at[2, e])

    for e in range(early):
        load_first(e).start()

    def fill(t, start, stop):
        for e in range(start, min(start + slots, stop)):
            load(t, e).start()

    def run(t, start, stop, last, body):
        @pl.loop(start, stop)
        def _(e):
            load(t, e).wait()
            body(e, lax.rem(e, slots))

            @pl.when(e + slots < last)
            def _():
                load(t, e + slots).start()

    fill(0, early, experts)
    weight_load = pltpu.make_async_copy(router_weight, weight, load_sem.at[3, 0])
    gain_load = pltpu.make_async_copy(router_gain, gain, load_sem.at[3, 1])
    weight_load.start()
    gain_load.start()

    barrier = pltpu.get_barrier_semaphore()
    for k in range(1, n):
        pl.semaphore_signal(barrier, inc=1, device_id={"rows": peer(k)}, device_id_type=MESH)
    for k in range(1, owners):
        pl.semaphore_signal(
            barrier, inc=1, device_id={"owner": lax.rem(home + k, owners)}, device_id_type=MESH
        )

    def put_part(t, e, sums):
        for q in range(half):
            part[q, t, pl.ds(e, 1), :] = sums[:, q * pair : (q + 1) * pair]

    def sums_wide(t):
        def body(e, slot):
            put_part(t, e, jnp.sum(jnp.abs(wide[slot]), axis=0, keepdims=True))

        return body

    def sums_tall(e, slot):
        for q in range(half):
            block = jnp.abs(tall[slot, q * pair : (q + 1) * pair, :])
            folded = block[:, :128]
            for c in range(128, rows, 128):
                folded = folded + block[:, c : c + 128]
            part[q, 2, pl.ds(e, 1), :] = jnp.sum(folded.T, axis=0, keepdims=True)

    for e in range(early):
        load_first(e).wait()
        sums = jnp.sum(jnp.abs(first[e]), axis=0, keepdims=True)
        put_part(0, e, sums)
        for s in range(2):
            early_part[s, e] = sums[:, s * (width // 2) : (s + 1) * (width // 2)]

    pl.semaphore_wait(barrier, n - 1 + owners - 1)

    inners = (half_chips - 1, half_chips)
    reach = [c * CORES + i for c in inners for i in range(CORES)]

    early_some = [pl.ds(0, 1)] + [pl.ds(1, early - 1)] * (early > 1)

    def early_copy(i, to, src):
        return remote(
            early_part.at[1 - to // half, early_some[i]],
            early_got.at[src, early_some[i]],
            early_send.at[i, to],
            early_recv.at[i, src],
            rows=to,
        )

    def early_sums(i):
        for to in reach:

            @pl.when(me != to)
            def _():
                early_copy(i, to, me).start()

    early_sums(0)

    raw = share % 128 == 0
    partner = across * CORES + core

    def raw_copy():
        return remote(
            first.at[0, :, pl.ds(pl.multiple_of(partner * share, share), share)],
            raw_got,
            raw_sem.at[0],
            raw_sem.at[1],
            rows=partner,
        )

    if raw:

        @pl.when(inner)
        def _():
            raw_copy().start()

    for i in range(1, len(early_some)):
        early_sums(i)

    weight_load.wait()
    gain_load.wait()
    router[...] = (weight[...] * gain[...]).astype(jnp.bfloat16)
    out_router[home, :, span] = router[...]

    def strip(src):
        return out_router.at[home, :, pl.ds(pl.multiple_of(src * rows, rows), rows)]

    def router_copy(to, src):
        return remote(router, strip(src), router_send.at[to], router_recv.at[src], rows=to)

    def forward_copy(to, src):
        return remote(
            strip(lax.rem(src + half, n)),
            strip(lax.rem(src + half, n)),
            fwd_send.at[to],
            fwd_recv.at[src],
            rows=to,
        )

    def col_copy(to, src):
        return remote(
            out_router.at[src], out_router.at[src], col_send.at[to], col_recv.at[src], owner=to
        )

    for k in range(1, half):
        router_copy(side * half + mate(k), me).start()
    router_copy(facing, me).start()

    shadow = min(early + SHADOW, experts)
    run(0, early, shadow, experts, sums_wide(0))

    stages = (pl.ds(0, 1), pl.ds(1, 2))

    def side_copy(s, to, src):
        return remote(
            part.at[to, stages[s]],
            got_side.at[src, stages[s]],
            side_send.at[s, to],
            side_recv.at[s, src],
            rows=side * half + to,
        )

    def half_copy(s):
        return remote(
            half_sum.at[stages[s]],
            got_half.at[stages[s]],
            half_send.at[s],
            half_recv.at[s],
            rows=facing,
        )

    def total_copy(s, to, src):
        block = total.at[src, stages[s]]
        return remote(
            block, block, total_send.at[s, to], total_recv.at[s, src], rows=side * half + to
        )

    def sums_side(s):
        for k in range(1, half):
            side_copy(s, mate(k), member).start()

    def sums_across(s):
        acc = part[member, stages[s]]
        for k in range(1, half):
            side_copy(s, mate(k), mate(k)).wait_recv()
            acc = acc + got_side[mate(k), stages[s]]
        half_sum[stages[s]] = acc
        half_copy(s).start()

    def sums_back(s):
        half_copy(s).wait_recv()
        total[member, stages[s]] = half_sum[stages[s]] + got_half[stages[s]]
        for k in range(1, half):
            total_copy(s, mate(k), member).start()

    scales = (scale_gate, scale_up, scale_down)

    def sums_done(s):
        for k in range(1, half):
            total_copy(s, mate(k), mate(k)).wait_recv()
        for t in ((0,), (1, 2))[s]:
            for q in range(half):
                inverse[q, t] = 1.0 / (total[q, t] / count)
            mine = total[me // 2, t] / count
            scales[t][...] = jnp.where(lax.rem(me, 2) == 0, mine[:, :share], mine[:, share:])

    def block_copy(t, g, to, src):
        start, size = groups[t][g]
        some = pl.ds(start, size)
        at = pl.ds(pl.multiple_of(src * rows, rows), rows)
        if t < 2:
            piece = send_wide.at[t, to, some]
            dst = (out_gate, out_up)[t].at[some, at, :]
        else:
            piece = send_tall.at[to, some]
            dst = out_down.at[some, :, at]
        b = base[t] + g
        return remote(piece, dst, bulk_send.at[b, to], bulk_recv.at[b, src], rows=to)

    def send_chip(t, g, there, cores=range(CORES)):
        for c in cores:
            block_copy(t, g, there * CORES + lax.rem(core + c, CORES), me).start()

    def send_side(t, g):
        for d in range(1, half_chips):
            for way in (1, -1):
                there = chip + way * d

                @pl.when((there // half_chips == chip // half_chips) & (there >= 0))
                def _():
                    send_chip(t, g, there)

        for c in range(1, CORES):
            block_copy(t, g, chip * CORES + lax.rem(core + c, CORES), me).start()

    last = (2, len(groups[2]) - 1)

    tail = (0, early - 1, half_chips - 1)
    tail_chip = jnp.where(side == 0, chips - 1, 0)
    tail_to = tail_chip * CORES + lax.rem(core + CORES - 1, CORES)

    def send_across(who, pieces):
        @pl.when(who)
        def _():
            for t, g, k in pieces:
                there = jnp.where(side == 0, half_chips + k, half_chips - 1 - k)
                if who is inner and (t, g, k) == tail:
                    send_chip(t, g, there, range(CORES - 1))
                else:
                    send_chip(t, g, there)

    def scaled_pair(t, e, q, block, factor):
        value = (block * factor).astype(jnp.bfloat16)
        for i in range(2):
            send_wide[t, 2 * q + i, e] = value[:, i * share : (i + 1) * share]

    def half_first(e, which, factor_of):
        for p in range(half // 2):
            q = which * (half // 2) + p
            at = pl.ds(pl.multiple_of(q * pair, pair), pair)
            scaled_pair(0, e, q, first[e, :, at], factor_of(p, q))

    def early_factor(e):
        return lambda p, q: early_inv[e, :, p * pair : (p + 1) * pair]

    def late_factor(e):
        return lambda p, q: inverse[q, 0, pl.ds(e, 1), :]

    def ready_wide(t):
        def body(e, slot):
            for q in range(half):
                scaled_pair(
                    t,
                    e,
                    q,
                    wide[slot, :, q * pair : (q + 1) * pair],
                    inverse[q, t, pl.ds(e, 1), :],
                )

        return body

    def ready_tall(e, slot):
        for q in range(half):
            row = inverse[q, 2, pl.ds(e, 1), :]
            factor = jnp.broadcast_to(row, (128, pair)).T
            for c in range(0, rows, 128):
                block = tall[slot, q * pair : (q + 1) * pair, c : c + 128]
                value = (block * factor).astype(jnp.bfloat16)
                for i in range(2):
                    send_tall[2 * q + i, e, :, c : c + 128] = value[
                        i * share : (i + 1) * share
                    ]

    def own(t, start, stop):
        @pl.loop(start, stop)
        def _(e):
            if t < 2:
                (out_gate, out_up)[t][e, span, :] = send_wide[t, me, e]
            else:
                out_down[e, :, span] = send_tall[me, e]

    def ready(t, g, last, body):
        start, size = groups[t][g]
        run(t, start, start + size, last, body)

    def early_inverse(i):
        @pl.when(inner)
        def _():
            acc = early_part[1 - side, early_some[i]]
            for k in range(1, n):
                early_copy(i, peer(k), peer(k)).wait_recv()
                acc = acc + early_got[peer(k), early_some[i]]
            early_inv[early_some[i]] = 1.0 / (acc / count)

    early_inverse(0)
    pieces = [(0, e, k) for k in range(half_chips) for e in range(early)]
    outer = jnp.logical_not(inner)
    middle = experts // 2
    rest = range(early, len(groups[0]))
    low = [g for g in rest if groups[0][g][0] < middle]
    high = [g for g in rest if groups[0][g][0] >= middle]

    def early_ready(e):
        @pl.when(inner)
        def _():
            half_first(e, 1 - side, early_factor(e))

    early_ready(0)
    if raw:

        @pl.when(inner)
        def _():
            send_chip(0, 0, across, range(1, CORES))

    send_across(inner, pieces[raw:1])
    run(0, shadow, experts, experts, sums_wide(0))
    fill(1, 0, middle)
    sums_side(0)
    for i in range(1, len(early_some)):
        early_inverse(i)
    for e in range(1, early):
        early_ready(e)
    send_across(inner, pieces[1:2])
    sums_across(0)
    send_across(inner, pieces[2:4])
    run(1, 0, middle, middle, sums_wide(1))
    fill(0, early, middle)
    fill(2, 0, experts)
    sums_back(0)
    send_across(inner, pieces[4:])
    sums_done(0)

    def next_group(g, stop):
        ready(0, g, stop, ready_wide(0))
        send_across(inner, [(0, g, 0)])
        send_side(0, g)

    for g in low:
        next_group(g, middle)
    fill(1, middle, experts)
    for e in range(early):
        half_first(e, side, late_factor(e))

        @pl.when(outer)
        def _():
            half_first(e, 1 - side, late_factor(e))

    for g in range(early):
        send_side(0, g)
    run(1, middle, experts, experts, sums_wide(1))
    fill(0, middle, experts)
    run(2, 0, experts, experts, sums_tall)
    fill(2, 0, experts)
    sums_side(1)
    for g in high[:1]:
        next_group(g, experts)
    sums_across(1)
    for g in high[1:]:
        next_group(g, experts)
    fill(1, 0, experts)
    sums_back(1)
    send_across(inner, [(0, g, k) for g in low for k in range(1, half_chips)])
    own(0, 0, experts)
    router_copy(facing, facing).wait_recv()
    for k in range(1, half):
        forward_copy(side * half + mate(k), me).start()
    sums_done(1)
    send_across(inner, [(0, g, k) for g in high for k in range(1, half_chips)])
    for t, body in ((1, ready_wide(1)), (2, ready_tall)):
        for g in range(len(groups[t])):
            ready(t, g, experts, body)
            send_across(inner, [(t, g, k) for k in range(half_chips) if (t, g, k) != (*last, 0)])
            send_side(t, g)

    start, size = groups[2][-1]
    for c in range(CORES):
        late_send[c] = send_tall[across * CORES + c, pl.ds(start, size)]
    for t in (1, 2):
        own(t, 0, experts)

    if raw:

        @pl.when(inner)
        def _():
            raw_copy().wait_recv()
            row = inverse[me // 2, 0, pl.ds(0, 1), :]
            mine = jnp.where(lax.rem(me, 2) == 0, row[:, :share], row[:, share:])
            at = pl.ds(pl.multiple_of(partner * rows, rows), rows)
            out_gate[0, at, :] = (raw_got[...] * mine).astype(jnp.bfloat16)
            raw_copy().wait_send()

    for k in range(1, half):
        other = side * half + mate(k)
        router_copy(other, other).wait_recv()
        forward_copy(other, other).wait_recv()
    for k in range(1, owners):
        col_copy(lax.rem(home + k, owners), home).start()

    @pl.when(inner)
    def _():
        send_chip(*tail[:2], tail_chip, range(CORES - 1, CORES))

    def kept(t, g, other):
        facing_chip = (other // CORES == across) & inner
        if (t, g) == last:
            return facing_chip
        if raw and (t, g) == (0, 0):
            return facing_chip & (other == partner)
        return None

    def unless(skip, body):
        if skip is None:
            body()
        else:
            pl.when(jnp.logical_not(skip))(body)

    outers = [c for c in range(half_chips - 1)]

    @pl.when(inner)
    def _():
        for t in range(3):
            for g in range(len(groups[t])):

                @pl.loop(0, half)
                def _(m):
                    other = (1 - side) * half + m
                    skip = kept(t, g, other)
                    if (t, g) == tail[:2]:
                        skip = (other == tail_to) if skip is None else skip | (other == tail_to)
                    unless(skip, lambda: block_copy(t, g, other, me).wait_send())

        for i in outers:
            there = jnp.where(side == 0, i, chips - 1 - i)
            for c in range(CORES):
                pl.semaphore_signal(
                    through, inc=1, device_id={"rows": there * CORES + c}, device_id_type=MESH
                )

        block_copy(*tail[:2], tail_to, me).wait_send()

    @pl.when(outer)
    def _():
        pl.semaphore_wait(through, CORES)

    for k in range(half_chips):
        send_across(outer, [(t, g, k) for t in range(3) for g in range(len(groups[t]))])

    for k in range(1, owners):
        other = lax.rem(home + k, owners)
        col_copy(other, other).wait_recv()
        col_copy(other, home).wait_send()
    router_copy(facing, me).wait_send()
    for k in range(1, half):
        other = side * half + mate(k)
        router_copy(other, me).wait_send()
        forward_copy(other, me).wait_send()
        for s in range(2):
            side_copy(s, mate(k), member).wait_send()
            total_copy(s, mate(k), member).wait_send()
    for s in range(2):
        half_copy(s).wait_send()
    for i in range(len(early_some)):
        for to in reach:

            @pl.when(me != to)
            def _():
                early_copy(i, to, me).wait_send()

    for t in range(3):
        for g in range(len(groups[t])):

            @pl.loop(1, n)
            def _(k):
                other = peer(k)
                unless(kept(t, g, other), lambda: block_copy(t, g, other, other).wait_recv())

                @pl.when(jnp.logical_not(inner & (other // half != side)))
                def _():
                    block_copy(t, g, other, me).wait_send()


def late_exchange(n, late_send, _, late_got, send_sem, recv_sem):
    me = lax.axis_index("rows")
    _, inner, across = sides(n, me)
    core = lax.rem(me, CORES)

    def copy(to, src):
        return pltpu.make_async_remote_copy(
            src_ref=late_send.at[to],
            dst_ref=late_got.at[src],
            send_sem=send_sem.at[to],
            recv_sem=recv_sem.at[src],
            device_id={"rows": across * CORES + to},
            device_id_type=MESH,
        )

    @pl.when(inner)
    def _():
        barrier = pltpu.get_barrier_semaphore()
        for c in range(CORES):
            pl.semaphore_signal(
                barrier, inc=1, device_id={"rows": across * CORES + c}, device_id_type=MESH
            )
        pl.semaphore_wait(barrier, CORES)
        for c in range(CORES):
            copy(lax.rem(core + c, CORES), core).start()
        for c in range(CORES):
            copy(c, c).wait_recv()
            copy(c, core).wait_send()


def late_place(n, start, late_got, down, out, sem):
    me = lax.axis_index("rows")
    _, inner, across = sides(n, me)
    size, rows = late_got.shape[1], late_got.shape[3]

    @pl.when(inner)
    def _():
        copies = []
        for c in range(CORES):
            src = across * CORES + c
            at = pl.ds(pl.multiple_of(src * rows, rows), rows)
            copies.append(
                pltpu.make_async_copy(
                    late_got.at[c], out.at[pl.ds(start, size), :, at], sem.at[c]
                )
            )
        for copy in copies:
            copy.start()
        for copy in copies:
            copy.wait()


def chunks_of(shape):
    count = CHUNKS if len(shape) == 3 and shape[0] % CHUNKS == 0 else 1
    size = shape[0] // count
    return [pl.ds(i * size, size) for i in range(count)]


def write_back(count, *refs):
    ins, outs, sem = refs[:count], refs[count : 2 * count], refs[2 * count]
    copies = []
    for i, (a, b) in enumerate(zip(ins, outs)):
        for j, some in enumerate(chunks_of(a.shape)):
            copies.append(pltpu.make_async_copy(a.at[some], b.at[some], sem.at[i, j]))
    for copy in copies:
        copy.start()
    for copy in copies:
        copy.wait()


def local(n, owners, gate, up, down, router_weight, router_gain):
    experts, rows, width = gate.shape
    share = width // n
    half = n // 2
    pair = 2 * share
    early, groups, _, total_groups = plan(experts)
    slots = min(SLOTS, experts)
    router = router_weight.T
    gain = router_gain.reshape(1, -1)
    columns = router.shape[0]
    anywhere = pl.BlockSpec(memory_space=pl.ANY)
    vmem = pl.BlockSpec(memory_space=pltpu.VMEM)
    hbm = pl.BlockSpec(memory_space=pltpu.HBM)
    f32, bf16 = jnp.float32, jnp.bfloat16
    dma = pltpu.SemaphoreType.DMA
    shapes = (
        ((experts, rows * n, share), bf16),
        ((experts, rows * n, share), bf16),
        ((experts, share, rows * n), bf16),
        ((experts, share), f32),
        ((experts, share), f32),
        ((experts, share), f32),
        ((owners, columns, rows * n), bf16),
    )
    start, size = groups[2][-1]
    late = ((CORES, size, share, rows), bf16)
    *results, late_send = pl.pallas_call(
        functools.partial(exchange, n, owners),
        name="exchange",
        out_shape=tuple(pltpu.VMEM(*s) for s in (*shapes, late)),
        in_specs=[anywhere] * 5,
        out_specs=(vmem,) * (len(shapes) + 1),
        scratch_shapes=[
            pltpu.VMEM((early, rows, width), f32),
            pltpu.VMEM((slots, rows, width), f32),
            pltpu.VMEM((slots, width, rows), f32),
            pltpu.VMEM((2, n, experts, rows, share), bf16),
            pltpu.VMEM((n, experts, share, rows), bf16),
            pltpu.VMEM((2, early, 1, width // 2), f32),
            pltpu.VMEM((n, early, 1, width // 2), f32),
            pltpu.VMEM((early, 1, width // 2), f32),
            pltpu.VMEM((rows, share), f32),
            pltpu.VMEM((half, 3, experts, pair), f32),
            pltpu.VMEM((half, 3, experts, pair), f32),
            pltpu.VMEM((3, experts, pair), f32),
            pltpu.VMEM((3, experts, pair), f32),
            pltpu.VMEM((half, 3, experts, pair), f32),
            pltpu.VMEM((half, 3, experts, pair), f32),
            pltpu.VMEM((columns, rows), f32),
            pltpu.VMEM((1, rows), f32),
            pltpu.VMEM((columns, rows), bf16),
            dma((4, max(slots, 2, early))),
            dma((2, n)),
            dma((2, n)),
            dma((2,)),
            dma((2, half)),
            dma((2, half)),
            dma((2,)),
            dma((2,)),
            dma((2, half)),
            dma((2, half)),
            dma((n,)),
            dma((n,)),
            dma((n,)),
            dma((n,)),
            dma((owners,)),
            dma((owners,)),
            dma((total_groups, n)),
            dma((total_groups, n)),
            pltpu.SemaphoreType.REGULAR,
        ],
        compiler_params=pltpu.CompilerParams(
            collective_id=0, has_side_effects=True, vmem_limit_bytes=38 * 1024 * 1024
        ),
    )(gate, up, down, router, gain)
    outs = pl.pallas_call(
        functools.partial(write_back, len(shapes)),
        name="write_back",
        out_shape=tuple(pltpu.HBM(*s) for s in shapes),
        in_specs=[vmem] * len(shapes),
        out_specs=(hbm,) * len(shapes),
        scratch_shapes=[dma((len(shapes), CHUNKS))],
        compiler_params=pltpu.CompilerParams(vmem_limit_bytes=1024 * 1024),
    )(*results)
    late_got = pl.pallas_call(
        functools.partial(late_exchange, n),
        name="late_exchange",
        out_shape=pltpu.VMEM(*late),
        in_specs=[vmem, anywhere],
        out_specs=vmem,
        scratch_shapes=[dma((CORES,)), dma((CORES,))],
        compiler_params=pltpu.CompilerParams(
            collective_id=1, has_side_effects=True, vmem_limit_bytes=1024 * 1024
        ),
    )(late_send, outs[3])
    ready_down = pl.pallas_call(
        functools.partial(late_place, n, start),
        name="late_place",
        out_shape=pltpu.HBM(*shapes[2]),
        in_specs=[vmem, hbm],
        out_specs=hbm,
        scratch_shapes=[dma((CORES,))],
        input_output_aliases={1: 0},
        compiler_params=pltpu.CompilerParams(vmem_limit_bytes=1024 * 1024),
    )(late_got, outs[2])
    serve_router = outs[6].reshape(owners * columns, rows * n).T
    return (*outs[:2], ready_down, *outs[3:6], serve_router)


def solution(mesh):
    return jax.shard_map(
        functools.partial(local, mesh.shape["rows"], mesh.shape["owner"]),
        mesh=mesh,
        in_specs=(
            P("owner", "rows", None),
            P("owner", "rows", None),
            P("owner", None, "rows"),
            P("rows", "owner"),
            P("rows"),
        ),
        out_specs=(
            P("owner", None, "rows"),
            P("owner", None, "rows"),
            P("owner", "rows", None),
            P("owner", "rows"),
            P("owner", "rows"),
            P("owner", "rows"),
            P(),
        ),
        check_vma=False,
    )
```

```python
import functools

import jax
import jax.numpy as jnp
from jax import lax
from jax.experimental import pallas as pl
from jax.experimental.pallas import tpu as pltpu
from jax.sharding import PartitionSpec as P

CORES = 2
SLOTS = 4
EARLY = 3
SHADOW = 11
CHUNKS = 4
GROUPS = 4
MESH = pl.DeviceIdType.MESH


def groups_of(experts, start):
    per = max(1, experts // GROUPS)
    out = [(e, 1) for e in range(start)]
    at = start
    while at < experts:
        end = min(experts, (at // per + 1) * per)
        out.append((at, end - at))
        at = end
    return out


def plan(experts):
    early = max(1, min(EARLY, experts // 4))
    groups = [groups_of(experts, early), groups_of(experts, 0), groups_of(experts, 0)]
    (start, size), (_, more) = groups[2][-2:]
    groups[2][-2:] = [(start, size + more)]
    base = [0, len(groups[0]), len(groups[0]) + len(groups[1])]
    return early, groups, base, sum(len(g) for g in groups)


def sides(n, me):
    chips = n // CORES
    chip = me // CORES
    inner = (chip == chips // 2 - 1) | (chip == chips // 2)
    return chip, inner, jnp.where(chip < chips // 2, chips // 2, chips // 2 - 1)


def exchange(
    n,
    owners,
    gate,
    up,
    down,
    router_weight,
    router_gain,
    out_gate,
    out_up,
    out_down,
    scale_gate,
    scale_up,
    scale_down,
    out_router,
    late_send,
    first,
    wide,
    tall,
    send_wide,
    send_tall,
    early_part,
    early_got,
    early_inv,
    raw_got,
    part,
    got_side,
    half_sum,
    got_half,
    total,
    inverse,
    weight,
    gain,
    router,
    load_sem,
    early_send,
    early_recv,
    raw_sem,
    side_send,
    side_recv,
    half_send,
    half_recv,
    total_send,
    total_recv,
    router_send,
    router_recv,
    fwd_send,
    fwd_recv,
    col_send,
    col_recv,
    bulk_send,
    bulk_recv,
    through,
):
    me = lax.axis_index("rows")
    home = lax.axis_index("owner")
    experts, rows, width = gate.shape
    share = width // n
    pair = 2 * share
    half = n // 2
    slots = wide.shape[0]
    chips = n // CORES
    half_chips = chips // 2
    chip, inner, across = sides(n, me)
    core = lax.rem(me, CORES)
    side = me // half
    member = lax.rem(me, half)
    facing = lax.rem(me + half, n)
    early, groups, base, _ = plan(experts)
    count = rows * n
    srcs = (gate, up, down)
    span = pl.ds(pl.multiple_of(me * rows, rows), rows)

    def peer(k):
        return lax.rem(me + k, n)

    def mate(k):
        return lax.rem(member + k, half)

    def remote(src, dst, out_sem, in_sem, **where):
        return pltpu.make_async_remote_copy(
            src_ref=src,
            dst_ref=dst,
            send_sem=out_sem,
            recv_sem=in_sem,
            device_id=where,
            device_id_type=MESH,
        )

    def load(t, e):
        buf = wide if t < 2 else tall
        slot = lax.rem(e, slots)
        return pltpu.make_async_copy(
            srcs[t].at[e], buf.at[slot], load_sem.at[0 if t < 2 else 1, slot]
        )

    def load_first(e):
        return pltpu.make_async_copy(gate.at[e], first.at[e], load_sem.at[2, e])

    for e in range(early):
        load_first(e).start()

    def fill(t, start, stop):
        for e in range(start, min(start + slots, stop)):
            load(t, e).start()

    def run(t, start, stop, last, body):
        @pl.loop(start, stop)
        def _(e):
            load(t, e).wait()
            body(e, lax.rem(e, slots))

            @pl.when(e + slots < last)
            def _():
                load(t, e + slots).start()

    fill(0, early, experts)
    weight_load = pltpu.make_async_copy(router_weight, weight, load_sem.at[3, 0])
    gain_load = pltpu.make_async_copy(router_gain, gain, load_sem.at[3, 1])
    weight_load.start()
    gain_load.start()

    barrier = pltpu.get_barrier_semaphore()
    for k in range(1, n):
        pl.semaphore_signal(barrier, inc=1, device_id={"rows": peer(k)}, device_id_type=MESH)
    for k in range(1, owners):
        pl.semaphore_signal(
            barrier, inc=1, device_id={"owner": lax.rem(home + k, owners)}, device_id_type=MESH
        )

    def put_part(t, e, sums):
        for q in range(half):
            part[q, t, pl.ds(e, 1), :] = sums[:, q * pair : (q + 1) * pair]

    def sums_wide(t):
        def body(e, slot):
            put_part(t, e, jnp.sum(jnp.abs(wide[slot]), axis=0, keepdims=True))

        return body

    def sums_tall(e, slot):
        for q in range(half):
            block = jnp.abs(tall[slot, q * pair : (q + 1) * pair, :])
            folded = block[:, :128]
            for c in range(128, rows, 128):
                folded = folded + block[:, c : c + 128]
            part[q, 2, pl.ds(e, 1), :] = jnp.sum(folded.T, axis=0, keepdims=True)

    for e in range(early):
        load_first(e).wait()
        sums = jnp.sum(jnp.abs(first[e]), axis=0, keepdims=True)
        put_part(0, e, sums)
        for s in range(2):
            early_part[s, e] = sums[:, s * (width // 2) : (s + 1) * (width // 2)]

    pl.semaphore_wait(barrier, n - 1 + owners - 1)

    inners = (half_chips - 1, half_chips)
    reach = [c * CORES + i for c in inners for i in range(CORES)]

    early_some = [pl.ds(0, 1)] + [pl.ds(1, early - 1)] * (early > 1)

    def early_copy(i, to, src):
        return remote(
            early_part.at[1 - to // half, early_some[i]],
            early_got.at[src, early_some[i]],
            early_send.at[i, to],
            early_recv.at[i, src],
            rows=to,
        )

    def early_sums(i):
        for to in reach:

            @pl.when(me != to)
            def _():
                early_copy(i, to, me).start()

    early_sums(0)

    raw = share % 128 == 0
    partner = across * CORES + core

    def raw_copy():
        return remote(
            first.at[0, :, pl.ds(pl.multiple_of(partner * share, share), share)],
            raw_got,
            raw_sem.at[0],
            raw_sem.at[1],
            rows=partner,
        )

    if raw:

        @pl.when(inner)
        def _():
            raw_copy().start()

    for i in range(1, len(early_some)):
        early_sums(i)

    weight_load.wait()
    gain_load.wait()
    router[...] = (weight[...] * gain[...]).astype(jnp.bfloat16)
    out_router[home, :, span] = router[...]

    def strip(src):
        return out_router.at[home, :, pl.ds(pl.multiple_of(src * rows, rows), rows)]

    def router_copy(to, src):
        return remote(router, strip(src), router_send.at[to], router_recv.at[src], rows=to)

    def forward_copy(to, src):
        return remote(
            strip(lax.rem(src + half, n)),
            strip(lax.rem(src + half, n)),
            fwd_send.at[to],
            fwd_recv.at[src],
            rows=to,
        )

    def col_copy(to, src):
        return remote(
            out_router.at[src], out_router.at[src], col_send.at[to], col_recv.at[src], owner=to
        )

    for k in range(1, half):
        router_copy(side * half + mate(k), me).start()
    router_copy(facing, me).start()

    shadow = min(early + SHADOW, experts)
    run(0, early, shadow, experts, sums_wide(0))

    stages = (pl.ds(0, 1), pl.ds(1, 2))

    def side_copy(s, to, src):
        return remote(
            part.at[to, stages[s]],
            got_side.at[src, stages[s]],
            side_send.at[s, to],
            side_recv.at[s, src],
            rows=side * half + to,
        )

    def half_copy(s):
        return remote(
            half_sum.at[stages[s]],
            got_half.at[stages[s]],
            half_send.at[s],
            half_recv.at[s],
            rows=facing,
        )

    def total_copy(s, to, src):
        block = total.at[src, stages[s]]
        return remote(
            block, block, total_send.at[s, to], total_recv.at[s, src], rows=side * half + to
        )

    def sums_side(s):
        for k in range(1, half):
            side_copy(s, mate(k), member).start()

    def sums_across(s):
        acc = part[member, stages[s]]
        for k in range(1, half):
            side_copy(s, mate(k), mate(k)).wait_recv()
            acc = acc + got_side[mate(k), stages[s]]
        half_sum[stages[s]] = acc
        half_copy(s).start()

    def sums_back(s):
        half_copy(s).wait_recv()
        total[member, stages[s]] = half_sum[stages[s]] + got_half[stages[s]]
        for k in range(1, half):
            total_copy(s, mate(k), member).start()

    scales = (scale_gate, scale_up, scale_down)

    def sums_done(s):
        for k in range(1, half):
            total_copy(s, mate(k), mate(k)).wait_recv()
        for t in ((0,), (1, 2))[s]:
            for q in range(half):
                inverse[q, t] = 1.0 / (total[q, t] / count)
            mine = total[me // 2, t] / count
            scales[t][...] = jnp.where(lax.rem(me, 2) == 0, mine[:, :share], mine[:, share:])

    def block_copy(t, g, to, src):
        start, size = groups[t][g]
        some = pl.ds(start, size)
        at = pl.ds(pl.multiple_of(src * rows, rows), rows)
        if t < 2:
            piece = send_wide.at[t, to, some]
            dst = (out_gate, out_up)[t].at[some, at, :]
        else:
            piece = send_tall.at[to, some]
            dst = out_down.at[some, :, at]
        b = base[t] + g
        return remote(piece, dst, bulk_send.at[b, to], bulk_recv.at[b, src], rows=to)

    def send_chip(t, g, there, cores=range(CORES)):
        for c in cores:
            block_copy(t, g, there * CORES + lax.rem(core + c, CORES), me).start()

    def send_side(t, g):
        for d in range(1, half_chips):
            for way in (1, -1):
                there = chip + way * d

                @pl.when((there // half_chips == chip // half_chips) & (there >= 0))
                def _():
                    send_chip(t, g, there)

        for c in range(1, CORES):
            block_copy(t, g, chip * CORES + lax.rem(core + c, CORES), me).start()

    last = (2, len(groups[2]) - 1)

    tail = (0, early - 1, half_chips - 1)
    tail_chip = jnp.where(side == 0, chips - 1, 0)
    tail_to = tail_chip * CORES + lax.rem(core + CORES - 1, CORES)

    def send_across(who, pieces):
        @pl.when(who)
        def _():
            for t, g, k in pieces:
                there = jnp.where(side == 0, half_chips + k, half_chips - 1 - k)
                if who is inner and (t, g, k) == tail:
                    send_chip(t, g, there, range(CORES - 1))
                else:
                    send_chip(t, g, there)

    def scaled_pair(t, e, q, block, factor):
        value = (block * factor).astype(jnp.bfloat16)
        for i in range(2):
            send_wide[t, 2 * q + i, e] = value[:, i * share : (i + 1) * share]

    def half_first(e, which, factor_of):
        for p in range(half // 2):
            q = which * (half // 2) + p
            at = pl.ds(pl.multiple_of(q * pair, pair), pair)
            scaled_pair(0, e, q, first[e, :, at], factor_of(p, q))

    def early_factor(e):
        return lambda p, q: early_inv[e, :, p * pair : (p + 1) * pair]

    def late_factor(e):
        return lambda p, q: inverse[q, 0, pl.ds(e, 1), :]

    def ready_wide(t):
        def body(e, slot):
            for q in range(half):
                scaled_pair(
                    t,
                    e,
                    q,
                    wide[slot, :, q * pair : (q + 1) * pair],
                    inverse[q, t, pl.ds(e, 1), :],
                )

        return body

    def ready_tall(e, slot):
        for q in range(half):
            row = inverse[q, 2, pl.ds(e, 1), :]
            factor = jnp.broadcast_to(row, (128, pair)).T
            for c in range(0, rows, 128):
                block = tall[slot, q * pair : (q + 1) * pair, c : c + 128]
                value = (block * factor).astype(jnp.bfloat16)
                for i in range(2):
                    send_tall[2 * q + i, e, :, c : c + 128] = value[
                        i * share : (i + 1) * share
                    ]

    def own(t, start, stop):
        @pl.loop(start, stop)
        def _(e):
            if t < 2:
                (out_gate, out_up)[t][e, span, :] = send_wide[t, me, e]
            else:
                out_down[e, :, span] = send_tall[me, e]

    def ready(t, g, last, body):
        start, size = groups[t][g]
        run(t, start, start + size, last, body)

    def early_inverse(i):
        @pl.when(inner)
        def _():
            acc = early_part[1 - side, early_some[i]]
            for k in range(1, n):
                early_copy(i, peer(k), peer(k)).wait_recv()
                acc = acc + early_got[peer(k), early_some[i]]
            early_inv[early_some[i]] = 1.0 / (acc / count)

    early_inverse(0)
    pieces = [(0, e, k) for k in range(half_chips) for e in range(early)]
    outer = jnp.logical_not(inner)
    middle = experts // 2
    rest = range(early, len(groups[0]))
    low = [g for g in rest if groups[0][g][0] < middle]
    high = [g for g in rest if groups[0][g][0] >= middle]

    def early_ready(e):
        @pl.when(inner)
        def _():
            half_first(e, 1 - side, early_factor(e))

    early_ready(0)
    if raw:

        @pl.when(inner)
        def _():
            send_chip(0, 0, across, range(1, CORES))

    send_across(inner, pieces[raw:1])
    run(0, shadow, experts, experts, sums_wide(0))
    fill(1, 0, middle)
    sums_side(0)
    for i in range(1, len(early_some)):
        early_inverse(i)
    for e in range(1, early):
        early_ready(e)
    send_across(inner, pieces[1:2])
    sums_across(0)
    send_across(inner, pieces[2:4])
    run(1, 0, middle, middle, sums_wide(1))
    fill(0, early, middle)
    fill(2, 0, experts)
    sums_back(0)
    send_across(inner, pieces[4:])
    sums_done(0)

    def next_group(g, stop):
        ready(0, g, stop, ready_wide(0))
        send_across(inner, [(0, g, 0)])
        send_side(0, g)

    for g in low:
        next_group(g, middle)
    fill(1, middle, experts)
    for e in range(early):
        half_first(e, side, late_factor(e))

        @pl.when(outer)
        def _():
            half_first(e, 1 - side, late_factor(e))

    for g in range(early):
        send_side(0, g)
    run(1, middle, experts, experts, sums_wide(1))
    fill(0, middle, experts)
    run(2, 0, experts, experts, sums_tall)
    fill(2, 0, experts)
    sums_side(1)
    for g in high[:1]:
        next_group(g, experts)
    sums_across(1)
    for g in high[1:]:
        next_group(g, experts)
    fill(1, 0, experts)
    sums_back(1)
    send_across(inner, [(0, g, k) for g in low for k in range(1, half_chips)])
    own(0, 0, experts)
    router_copy(facing, facing).wait_recv()
    for k in range(1, half):
        forward_copy(side * half + mate(k), me).start()
    sums_done(1)
    send_across(inner, [(0, g, k) for g in high for k in range(1, half_chips)])
    for t, body in ((1, ready_wide(1)), (2, ready_tall)):
        for g in range(len(groups[t])):
            ready(t, g, experts, body)
            send_across(inner, [(t, g, k) for k in range(half_chips) if (t, g, k) != (*last, 0)])
            send_side(t, g)

    start, size = groups[2][-1]
    for c in range(CORES):
        late_send[c] = send_tall[across * CORES + c, pl.ds(start, size)]
    for t in (1, 2):
        own(t, 0, experts)

    if raw:

        @pl.when(inner)
        def _():
            raw_copy().wait_recv()
            row = inverse[me // 2, 0, pl.ds(0, 1), :]
            mine = jnp.where(lax.rem(me, 2) == 0, row[:, :share], row[:, share:])
            at = pl.ds(pl.multiple_of(partner * rows, rows), rows)
            out_gate[0, at, :] = (raw_got[...] * mine).astype(jnp.bfloat16)
            raw_copy().wait_send()

    for k in range(1, half):
        other = side * half + mate(k)
        router_copy(other, other).wait_recv()
        forward_copy(other, other).wait_recv()
    for k in range(1, owners):
        col_copy(lax.rem(home + k, owners), home).start()

    @pl.when(inner)
    def _():
        send_chip(*tail[:2], tail_chip, range(CORES - 1, CORES))

    def kept(t, g, other):
        facing_chip = (other // CORES == across) & inner
        if (t, g) == last:
            return facing_chip
        if raw and (t, g) == (0, 0):
            return facing_chip & (other == partner)
        return None

    def unless(skip, body):
        if skip is None:
            body()
        else:
            pl.when(jnp.logical_not(skip))(body)

    outers = [c for c in range(half_chips - 1)]

    @pl.when(inner)
    def _():
        for t in range(3):
            for g in range(len(groups[t])):

                @pl.loop(0, half)
                def _(m):
                    other = (1 - side) * half + m
                    skip = kept(t, g, other)
                    if (t, g) == tail[:2]:
                        skip = (other == tail_to) if skip is None else skip | (other == tail_to)
                    unless(skip, lambda: block_copy(t, g, other, me).wait_send())

        for i in outers:
            there = jnp.where(side == 0, i, chips - 1 - i)
            for c in range(CORES):
                pl.semaphore_signal(
                    through, inc=1, device_id={"rows": there * CORES + c}, device_id_type=MESH
                )

        block_copy(*tail[:2], tail_to, me).wait_send()

    @pl.when(outer)
    def _():
        pl.semaphore_wait(through, CORES)

    for k in range(half_chips):
        send_across(outer, [(t, g, k) for t in range(3) for g in range(len(groups[t]))])

    for k in range(1, owners):
        other = lax.rem(home + k, owners)
        col_copy(other, other).wait_recv()
        col_copy(other, home).wait_send()
    router_copy(facing, me).wait_send()
    for k in range(1, half):
        other = side * half + mate(k)
        router_copy(other, me).wait_send()
        forward_copy(other, me).wait_send()
        for s in range(2):
            side_copy(s, mate(k), member).wait_send()
            total_copy(s, mate(k), member).wait_send()
    for s in range(2):
        half_copy(s).wait_send()
    for i in range(len(early_some)):
        for to in reach:

            @pl.when(me != to)
            def _():
                early_copy(i, to, me).wait_send()

    for t in range(3):
        for g in range(len(groups[t])):

            @pl.loop(1, n)
            def _(k):
                other = peer(k)
                unless(kept(t, g, other), lambda: block_copy(t, g, other, other).wait_recv())

                @pl.when(jnp.logical_not(inner & (other // half != side)))
                def _():
                    block_copy(t, g, other, me).wait_send()


def late_exchange(n, late_send, _, late_got, send_sem, recv_sem):
    me = lax.axis_index("rows")
    _, inner, across = sides(n, me)
    core = lax.rem(me, CORES)

    def copy(to, src):
        return pltpu.make_async_remote_copy(
            src_ref=late_send.at[to],
            dst_ref=late_got.at[src],
            send_sem=send_sem.at[to],
            recv_sem=recv_sem.at[src],
            device_id={"rows": across * CORES + to},
            device_id_type=MESH,
        )

    @pl.when(inner)
    def _():
        barrier = pltpu.get_barrier_semaphore()
        for c in range(CORES):
            pl.semaphore_signal(
                barrier, inc=1, device_id={"rows": across * CORES + c}, device_id_type=MESH
            )
        pl.semaphore_wait(barrier, CORES)
        for c in range(CORES):
            copy(lax.rem(core + c, CORES), core).start()
        for c in range(CORES):
            copy(c, c).wait_recv()
            copy(c, core).wait_send()


def late_place(n, start, late_got, down, out, sem):
    me = lax.axis_index("rows")
    _, inner, across = sides(n, me)
    size, rows = late_got.shape[1], late_got.shape[3]

    @pl.when(inner)
    def _():
        copies = []
        for c in range(CORES):
            src = across * CORES + c
            at = pl.ds(pl.multiple_of(src * rows, rows), rows)
            copies.append(
                pltpu.make_async_copy(
                    late_got.at[c], out.at[pl.ds(start, size), :, at], sem.at[c]
                )
            )
        for copy in copies:
            copy.start()
        for copy in copies:
            copy.wait()


def chunks_of(shape):
    count = CHUNKS if len(shape) == 3 and shape[0] % CHUNKS == 0 else 1
    size = shape[0] // count
    return [pl.ds(i * size, size) for i in range(count)]


def write_back(count, *refs):
    ins, outs, sem = refs[:count], refs[count : 2 * count], refs[2 * count]
    copies = []
    for i, (a, b) in enumerate(zip(ins, outs)):
        for j, some in enumerate(chunks_of(a.shape)):
            copies.append(pltpu.make_async_copy(a.at[some], b.at[some], sem.at[i, j]))
    for copy in copies:
        copy.start()
    for copy in copies:
        copy.wait()


def local(n, owners, gate, up, down, router_weight, router_gain):
    experts, rows, width = gate.shape
    share = width // n
    half = n // 2
    pair = 2 * share
    early, groups, _, total_groups = plan(experts)
    slots = min(SLOTS, experts)
    router = router_weight.T
    gain = router_gain.reshape(1, -1)
    columns = router.shape[0]
    anywhere = pl.BlockSpec(memory_space=pl.ANY)
    vmem = pl.BlockSpec(memory_space=pltpu.VMEM)
    hbm = pl.BlockSpec(memory_space=pltpu.HBM)
    f32, bf16 = jnp.float32, jnp.bfloat16
    dma = pltpu.SemaphoreType.DMA
    shapes = (
        ((experts, rows * n, share), bf16),
        ((experts, rows * n, share), bf16),
        ((experts, share, rows * n), bf16),
        ((experts, share), f32),
        ((experts, share), f32),
        ((experts, share), f32),
        ((owners, columns, rows * n), bf16),
    )
    start, size = groups[2][-1]
    late = ((CORES, size, share, rows), bf16)
    *results, late_send = pl.pallas_call(
        functools.partial(exchange, n, owners),
        name="exchange",
        out_shape=tuple(pltpu.VMEM(*s) for s in (*shapes, late)),
        in_specs=[anywhere] * 5,
        out_specs=(vmem,) * (len(shapes) + 1),
        scratch_shapes=[
            pltpu.VMEM((early, rows, width), f32),
            pltpu.VMEM((slots, rows, width), f32),
            pltpu.VMEM((slots, width, rows), f32),
            pltpu.VMEM((2, n, experts, rows, share), bf16),
            pltpu.VMEM((n, experts, share, rows), bf16),
            pltpu.VMEM((2, early, 1, width // 2), f32),
            pltpu.VMEM((n, early, 1, width // 2), f32),
            pltpu.VMEM((early, 1, width // 2), f32),
            pltpu.VMEM((rows, share), f32),
            pltpu.VMEM((half, 3, experts, pair), f32),
            pltpu.VMEM((half, 3, experts, pair), f32),
            pltpu.VMEM((3, experts, pair), f32),
            pltpu.VMEM((3, experts, pair), f32),
            pltpu.VMEM((half, 3, experts, pair), f32),
            pltpu.VMEM((half, 3, experts, pair), f32),
            pltpu.VMEM((columns, rows), f32),
            pltpu.VMEM((1, rows), f32),
            pltpu.VMEM((columns, rows), bf16),
            dma((4, max(slots, 2, early))),
            dma((2, n)),
            dma((2, n)),
            dma((2,)),
            dma((2, half)),
            dma((2, half)),
            dma((2,)),
            dma((2,)),
            dma((2, half)),
            dma((2, half)),
            dma((n,)),
            dma((n,)),
            dma((n,)),
            dma((n,)),
            dma((owners,)),
            dma((owners,)),
            dma((total_groups, n)),
            dma((total_groups, n)),
            pltpu.SemaphoreType.REGULAR,
        ],
        compiler_params=pltpu.CompilerParams(
            collective_id=0, has_side_effects=True, vmem_limit_bytes=38 * 1024 * 1024
        ),
    )(gate, up, down, router, gain)
    outs = pl.pallas_call(
        functools.partial(write_back, len(shapes)),
        name="write_back",
        out_shape=tuple(pltpu.HBM(*s) for s in shapes),
        in_specs=[vmem] * len(shapes),
        out_specs=(hbm,) * len(shapes),
        scratch_shapes=[dma((len(shapes), CHUNKS))],
        compiler_params=pltpu.CompilerParams(vmem_limit_bytes=1024 * 1024),
    )(*results)
    late_got = pl.pallas_call(
        functools.partial(late_exchange, n),
        name="late_exchange",
        out_shape=pltpu.VMEM(*late),
        in_specs=[vmem, anywhere],
        out_specs=vmem,
        scratch_shapes=[dma((CORES,)), dma((CORES,))],
        compiler_params=pltpu.CompilerParams(
            collective_id=1, has_side_effects=True, vmem_limit_bytes=1024 * 1024
        ),
    )(late_send, outs[3])
    ready_down = pl.pallas_call(
        functools.partial(late_place, n, start),
        name="late_place",
        out_shape=pltpu.HBM(*shapes[2]),
        in_specs=[vmem, hbm],
        out_specs=hbm,
        scratch_shapes=[dma((CORES,))],
        input_output_aliases={1: 0},
        compiler_params=pltpu.CompilerParams(vmem_limit_bytes=1024 * 1024),
    )(late_got, outs[2])
    serve_router = outs[6].reshape(owners * columns, rows * n).T
    return (*outs[:2], ready_down, *outs[3:6], serve_router)


def solution(mesh):
    return jax.shard_map(
        functools.partial(local, mesh.shape["rows"], mesh.shape["owner"]),
        mesh=mesh,
        in_specs=(
            P("owner", "rows", None),
            P("owner", "rows", None),
            P("owner", None, "rows"),
            P("rows", "owner"),
            P("rows"),
        ),
        out_specs=(
            P("owner", None, "rows"),
            P("owner", None, "rows"),
            P("owner", "rows", None),
            P("owner", "rows"),
            P("owner", "rows"),
            P("owner", "rows"),
            P(),
        ),
        check_vma=False,
    )
```
